128 devices in a mesh: sample: 2 (over x_hi), space: 64 (over x_lo, y, z, core).
Axes of the slice: x: 4 (x_hi: 2, x_lo: 2; x = x_hi * 2 + x_lo), y: 4, z: 4, core: 2. Of those that a mesh axis runs over, the one named last changes fastest.
Arguments:
- volumes: bfloat16 [2, 256, 16, 64, 128], P('sample', 'space'), may hold values from -6 to 6
- fine_kernel: bfloat16 [27, 128, 128], replicated, may hold values from -0.109375 to 0.109375
- coarse_kernel: bfloat16 [27, 128, 256], replicated, may hold values from -0.109375 to 0.109375
- cotangent: bfloat16 [2, 128, 8, 32, 256], P('sample', 'space'), may hold values from -6 to 6
Outputs:
- coarse_out: bfloat16 [2, 128, 8, 32, 256], P('sample', 'space')
- fine_grad: float32 [128, 3456], P('space')
- coarse_grad: float32 [256, 3456], P('space')
The draws below stay inside these ranges and needn't reach their ends.
All inputs are finite; a program needn't handle non-finite values.
Results may differ from the reference program's by a relative error of at most 0.014.
Values may be sent and summed in bfloat16 or wider, within the bound.
A program may use at most 128 MiB of HBM per device.

```python
import jax
import jax.numpy as jnp
from jax import lax

C1 = 128
C2 = 256
NY = 16
NZ = 64
SAMPLES = 2
NX = 256


def level_of(rng, extent, split, low, top_value):
    loudness, own = 1.0, jax.random.fold_in(rng, 6)
    for axis_at, shards_of in split:
        heights = jnp.exp(jax.random.uniform(jax.random.fold_in(own, axis_at), (shards_of,), jnp.float32, low / len(split), top_value / len(split)))
        loudness = loudness * jnp.repeat(heights, extent[axis_at] // shards_of).reshape([-1 if axis == axis_at else 1 for axis in range(len(extent))])
    return loudness


def normal_values(rng, shape, width, reach, shards=(), kind=jnp.bfloat16):
    factor_of = level_of(rng, shape, shards, -0.22, 0.18) if shards else 1.0
    result = jax.random.normal(rng, shape, jnp.float32) * width * factor_of
    return jnp.minimum(jnp.maximum(result, -reach), reach).astype(kind)


def setup_inputs(seed: int = 0) -> dict:
    splits = jax.random.split(jax.random.key(seed), 5)
    volumes = normal_values(splits[0], (SAMPLES, NX, NY, NZ, C1), 1.0, 6.0, ((0, 2), (1, 64)))
    fine_kernel = normal_values(splits[1], (27, C1, C1), (27 * C1) ** -0.5, 0.109375)
    coarse_kernel = normal_values(splits[2], (27, C1, C2), (27 * C1) ** -0.5, 0.109375)
    cotangent = normal_values(splits[3], (SAMPLES, NX // 2, NY // 2, NZ // 2, C2), 1.0, 6.0, ((0, 2), (1, 64)))
    return dict(volumes=volumes, fine_kernel=fine_kernel, coarse_kernel=coarse_kernel, cotangent=cotangent)


def silu_slope(value):
    sig = jax.nn.sigmoid(value)
    return sig * (1.0 + value * (1.0 - sig))


def shifted(padded, tap, shape):
    first = (tap // 9).astype(jnp.int32)
    second = ((tap // 3) % 3).astype(jnp.int32)
    third = (tap % 3).astype(jnp.int32)
    anchor = jnp.zeros((), jnp.int32)
    piece = lax.dynamic_slice(padded, (first, second, third, anchor), (shape[0], shape[1], shape[2], padded.shape[3]))
    return piece.reshape(-1, padded.shape[-1])


def tap_list():
    return jnp.arange(27, dtype=jnp.int32)


def forward_taps(field, kernel):
    shape = field.shape[:3]
    padded = jnp.pad(field, ((1, 1), (1, 1), (1, 1), (0, 0)))
    start = jnp.zeros((shape[0] * shape[1] * shape[2], kernel.shape[2]), jnp.float32)

    def step(total, inputs):
        tap, weight = inputs
        total = total + jnp.dot(shifted(padded, tap, shape), weight, preferred_element_type=jnp.float32)
        return total, None

    total, unused = lax.scan(step, start, (tap_list(), kernel))
    return total, padded


def backward_taps(delta, kernel):
    shape = delta.shape[:3]
    padded = jnp.pad(delta, ((1, 1), (1, 1), (1, 1), (0, 0)))
    start = jnp.zeros((shape[0] * shape[1] * shape[2], kernel.shape[1]), jnp.float32)

    def step(total, inputs):
        tap, weight = inputs
        flipped = (26 - tap).astype(jnp.int32)
        total = total + lax.dot_general(shifted(padded, flipped, shape), weight, (((1,), (1,)), ((), ())), preferred_element_type=jnp.float32)
        return total, None

    total, unused = lax.scan(step, start, (tap_list(), kernel))
    return total


def kernel_term(delta_rows, padded, shape):
    def step(carry, tap):
        piece = lax.dot_general(delta_rows, shifted(padded, tap, shape), (((0,), (0,)), ((), ())), preferred_element_type=jnp.float32)
        return carry, piece

    unused, pieces = lax.scan(step, jnp.zeros((), jnp.float32), tap_list())
    return jnp.moveaxis(pieces, 0, 1).reshape(pieces.shape[1], -1)


def reference(volumes, fine_kernel, coarse_kernel, cotangent):
    outputs = []
    fine_total = jnp.zeros((fine_kernel.shape[2], 27 * fine_kernel.shape[1]), jnp.float32)
    coarse_total = jnp.zeros((coarse_kernel.shape[2], 27 * coarse_kernel.shape[1]), jnp.float32)
    for index in range(volumes.shape[0]):
        field = volumes[index]
        fx, fy, fz, chan = field.shape
        fine_pre, fine_pad = forward_taps(field, fine_kernel)
        fine_act = jax.nn.silu(fine_pre).astype(jnp.bfloat16)
        blocks = fine_act.astype(jnp.float32).reshape(fx // 2, 2, fy // 2, 2, fz // 2, 2, chan)
        pooled = jnp.mean(blocks, axis=(1, 3, 5)).astype(jnp.bfloat16)
        coarse_pre, coarse_pad = forward_taps(pooled, coarse_kernel)
        outputs.append(jax.nn.silu(coarse_pre).astype(jnp.bfloat16).reshape(fx // 2, fy // 2, fz // 2, -1))
        grad_rows = cotangent[index].reshape(-1, coarse_kernel.shape[2]).astype(jnp.float32)
        coarse_delta = (grad_rows * silu_slope(coarse_pre)).astype(jnp.bfloat16)
        pooled_grad = backward_taps(coarse_delta.reshape(fx // 2, fy // 2, fz // 2, -1), coarse_kernel).astype(jnp.bfloat16)
        spread = pooled_grad.astype(jnp.float32).reshape(fx // 2, fy // 2, fz // 2, chan) / 8.0
        spread = jnp.repeat(jnp.repeat(jnp.repeat(spread, 2, axis=0), 2, axis=1), 2, axis=2)
        fine_delta = (spread.reshape(-1, chan) * silu_slope(fine_pre)).astype(jnp.bfloat16)
        fine_total = fine_total + kernel_term(fine_delta, fine_pad, (fx, fy, fz))
        coarse_total = coarse_total + kernel_term(coarse_delta, coarse_pad, (fx // 2, fy // 2, fz // 2))
    return jnp.stack(outputs), fine_total, coarse_total
```

```python
import functools

import jax
import jax.numpy as jnp
from jax import lax
from jax.experimental import pallas as pl
from jax.experimental.pallas import tpu as pltpu
from jax.sharding import PartitionSpec as P

F32 = jnp.float32
BF16 = jnp.bfloat16
MESH = pl.DeviceIdType.MESH
NT = (((1,), (1,)), ((), ()))

COARSE_UNITS = (("z", tuple(range(14))), ("y", tuple(range(14, 27))))
FINE_UNITS = (
    ("z", ((0, 0), (0, 1), (0, 2), (1, 0))),
    ("y", ((1, 1), (1, 2), (2, 0))),
    ("z", ((2, 1), (2, 2))),
)


def fine_taps(groups):
    return tuple(9 * a + 3 * b + c for a, c in groups for b in range(3))


def mm(x, w):
    return jnp.dot(x, w, preferred_element_type=F32)


def mm_nt(x, w):
    return lax.dot_general(x, w, NT, preferred_element_type=F32)


def sigmoid(v):
    return 1.0 / (1.0 + jnp.exp(-v))


def up16(n):
    return -(-n // 16) * 16


def place():
    s = lax.axis_index("sample")
    i = lax.axis_index("space")
    return s, i // 32, (i // 8) % 4, (i // 2) % 4, i % 2


def device(s, xl, y, z, core):
    return (s, ((xl * 4 + y) * 4 + z) * 2 + core)


def moved(ds, dxl, dy, dz, dcore):
    s, xl, y, z, core = place()
    return device(
        (s + ds) % 2, (xl + dxl) % 2, (y + dy) % 4, (z + dz) % 4, (core + dcore) % 2
    )


def b_moves():
    return [
        (do, dxl, ds) for do in range(4) for dxl in range(2) for ds in range(2)
    ]


def permutation(rows, first, width):
    s, xl, y, z, core = place()
    m = lax.broadcasted_iota(jnp.int32, (rows, width), 0)
    o = lax.broadcasted_iota(jnp.int32, (rows, width), 1)
    r = width // 64
    group = m // r
    mxl = (group % 2 + xl) % 2
    other = (group // 2) % 4
    lead = (group // 8) % 4
    mcore = ((group // 32) % 2 + core) % 2
    if first == "z":
        mz, my = (lead + z) % 4, (other + y) % 4
    else:
        mz, my = (other + z) % 4, (lead + y) % 4
    shard = ((mxl * 4 + my) * 4 + mz) * 2 + mcore
    return (shard * r + m % r == o).astype(F32).astype(BF16)


class Unit:
    def __init__(self, index, first, taps, rows, refs):
        self.index, self.first, self.taps, self.rows = index, first, taps, rows
        (self.own, self.send0, self.recv0, self.keep, self.senda, self.recva,
         self.sendb, self.recvb, self.sem0, self.sema, self.semb) = refs
        self.half = 32 * rows
        self.chunk = 8 * rows
        self.fold = up16(len(taps) * rows)

    def put(self, j, value):
        lanes = pl.ds(j * 128, 128)
        self.own[:, lanes] = value[: self.half]
        self.send0[:, lanes] = value[self.half :].astype(BF16)

    def core_copy(self):
        return pltpu.make_async_remote_copy(
            self.send0, self.recv0, self.sem0.at[0], self.sem0.at[1],
            device_id=moved(0, 0, 0, 0, 1), device_id_type=MESH,
        )

    def lead(self, d):
        return moved(0, 0, 0, d, 0) if self.first == "z" else moved(0, 0, d, 0, 0)

    def a_copy(self, d):
        return pltpu.make_async_remote_copy(
            self.senda.at[d - 1], self.recva.at[d - 1],
            self.sema.at[0, d - 1], self.sema.at[1, d - 1],
            device_id=self.lead(d), device_id_type=MESH,
        )

    def b_copy(self, move):
        do, dxl, ds = move
        slot = do * 4 + dxl * 2 + ds - 1
        to = moved(ds, dxl, do, 0, 0) if self.first == "z" else moved(ds, dxl, 0, do, 0)
        return pltpu.make_async_remote_copy(
            self.sendb.at[do * 2 + dxl], self.recvb.at[slot],
            self.semb.at[0, slot], self.semb.at[1, slot],
            device_id=to, device_id_type=MESH,
        )

    def step_core(self):
        self.core_copy().start()

    def step_a(self):
        self.core_copy().wait()
        total = self.own[...] + self.recv0[...].astype(F32)
        self.keep[...] = total[: self.chunk]
        for d in range(1, 4):
            self.senda[d - 1] = total[d * self.chunk : (d + 1) * self.chunk].astype(BF16)
        for d in (2, 1, 3):
            self.a_copy(d).start()

    def step_b(self):
        total = self.keep[...]
        for d in range(1, 4):
            self.a_copy(d).wait()
        for d in range(1, 4):
            total = total + self.recva[d - 1].astype(F32)
        r = self.rows
        for q in range(8):
            rows = total[q * r : (q + 1) * r]
            pieces = [rows[:, j * 128 : (j + 1) * 128] for j in range(len(self.taps))]
            missing = self.fold - r * len(self.taps)
            if missing:
                pieces.append(jnp.zeros((missing, 128), F32))
            self.sendb[q] = jnp.concatenate(pieces, axis=0).astype(BF16)
        moves = b_moves()[1:]
        for move in sorted(moves, key=lambda m: -(m[0] % 2 + 2 * (m[0] == 2) + m[1] + 2 * m[2])):
            self.b_copy(move).start()

    def step_c(self, out):
        for move in b_moves()[1:]:
            self.b_copy(move).wait()
        total = None
        for do in range(4):
            for dxl in range(2):
                slot = do * 4 + dxl * 2 - 1
                near = self.sendb[0] if slot < 0 else self.recvb[slot]
                pair = near.astype(F32) + self.recvb[slot + 1].astype(F32)
                total = pair if total is None else total + pair
        r = self.rows
        for j, tap in enumerate(self.taps):
            out[:, tap * 128 : (tap + 1) * 128] = total[j * r : (j + 1) * r]


def unit_scratch(taps, rows):
    width, half, chunk = len(taps) * 128, 32 * rows, 8 * rows
    fold = up16(len(taps) * rows)
    return [
        pltpu.VMEM((half, width), F32),
        pltpu.VMEM((half, width), BF16),
        pltpu.VMEM((half, width), BF16),
        pltpu.VMEM((chunk, width), F32),
        pltpu.VMEM((3, chunk, width), BF16),
        pltpu.VMEM((3, chunk, width), BF16),
        pltpu.VMEM((8, fold, 128), BF16),
        pltpu.VMEM((15, fold, 128), BF16),
        pltpu.SemaphoreType.DMA((2,)),
        pltpu.SemaphoreType.DMA((2, 3)),
        pltpu.SemaphoreType.DMA((2, 15)),
    ]


def shift_rows(block, step, period):
    size = block.shape[0]
    row = lax.broadcasted_iota(jnp.int32, block.shape, 0) % period
    if step > 0:
        return jnp.where(row == 0, 0.0, pltpu.roll(block, 1, 0))
    return jnp.where(row == period - 1, 0.0, pltpu.roll(block, size - 1, 0))


def kernel(
    vol, fk_hbm, ck_hbm, ct_hbm,
    out_hbm, fine_out, coarse_out,
    v, fk, ck, ct, slope, pool, spr, pc, cd, cacc, outb, dt,
    sem_in, sem_out, sem_v, sem_p, sem_c,
    *unit_refs,
):
    s, i = lax.axis_index("sample"), lax.axis_index("space")
    left = (s, (i + 63) % 64)
    right = (s, (i + 1) % 64)
    units = []
    at = 0
    for index, (first, taps) in enumerate(COARSE_UNITS):
        units.append(Unit(index, first, taps, 4, unit_refs[at : at + 11]))
        at += 11
    for index, (first, groups) in enumerate(FINE_UNITS):
        units.append(Unit(index, first, fine_taps(groups), 2, unit_refs[at : at + 11]))
        at += 11
    coarse_units, fine_units = units[: len(COARSE_UNITS)], units[len(COARSE_UNITS) :]

    barrier = pltpu.get_barrier_semaphore()
    moves = {(ds, dxl, do, 0, 0) for do, dxl, ds in b_moves()}
    moves |= {(ds, dxl, 0, do, 0) for do, dxl, ds in b_moves()}
    moves.discard((0, 0, 0, 0, 0))
    moves.add((0, 0, 0, 0, 1))
    peers = [moved(*move) for move in sorted(moves)] + [left, right]
    for peer in peers:
        pl.semaphore_signal(barrier, inc=1, device_id=peer, device_id_type=MESH)

    def interior(e):
        return pltpu.make_async_copy(
            vol.at[:, :, e],
            v.at[1, pl.ds(1, 4), pl.ds(1, 8), :, pl.ds(e * 128, 128)],
            sem_in.at[e],
        )

    load_fk = pltpu.make_async_copy(fk_hbm, fk, sem_in.at[2])
    load_ck = pltpu.make_async_copy(ck_hbm, ck, sem_in.at[3])
    load_ct = pltpu.make_async_copy(ct_hbm, ct, sem_in.at[4])
    interior(0).start()
    interior(1).start()
    load_fk.start()
    load_ck.start()
    load_ct.start()

    def halo(side, e):
        return pltpu.make_async_remote_copy(
            vol.at[3 if side == 0 else 0, :, e],
            v.at[1, 0 if side == 0 else 5, pl.ds(1, 8), :, pl.ds(e * 128, 128)],
            sem_v.at[0, side, e], sem_v.at[1, side, e],
            device_id=right if side == 0 else left, device_id_type=MESH,
        )

    for c in range(3):
        for p in range(6):
            v[c, p, 0] = jnp.zeros((64, 256), BF16)
            v[c, p, 9] = jnp.zeros((64, 256), BF16)
        for p in range(4):
            pc[c, p, 0] = jnp.zeros((32, 128), BF16)
            pc[c, p, 9] = jnp.zeros((32, 128), BF16)
    for p in range(4):
        cd[p, 0] = jnp.zeros((32, 256), BF16)
        cd[p, 9] = jnp.zeros((32, 256), BF16)

    pl.semaphore_wait(barrier, len(peers))
    for side in range(2):
        for e in range(2):
            halo(side, e).start()

    def shift_fine(p):
        block = v[1, p, 1:9].reshape(512, 256).astype(F32)
        v[0, p, 1:9] = shift_rows(block, 1, 64).astype(BF16).reshape(8, 64, 256)
        v[2, p, 1:9] = shift_rows(block, -1, 64).astype(BF16).reshape(8, 64, 256)

    interior(0).wait()
    interior(1).wait()
    for p in range(1, 5):
        shift_fine(p)
    load_fk.wait()

    zero = jnp.zeros((128, 128), BF16)

    def beside(a, b):
        return jnp.concatenate([a, b], axis=1)

    def over(a, b):
        return jnp.concatenate([a, b], axis=0)

    def fine_forward(p):
        acc = None
        for a in range(3):
            for c in range(3):
                k0, k1, k2 = (fk[9 * a + 3 * b + c] for b in range(3))
                here = v[c, p + a, 1:9].reshape(512, 256)
                around = beside(
                    v[c, p + a, 0:8, :, 128:256].reshape(512, 128),
                    v[c, p + a, 2:10, :, 0:128].reshape(512, 128),
                )
                term = mm(here, over(beside(k1, k0), beside(k2, k1)))
                term = term + mm(around, over(beside(k0, zero), beside(zero, k2)))
                acc = term if acc is None else acc + term
        sig = sigmoid(acc)
        act = acc * sig
        slope[p] = sig + act * (1.0 - sig)
        return act[:, :128] + act[:, 128:]

    def shift_pooled(p):
        block = pc[1, p, 1:9].reshape(256, 128).astype(F32)
        pc[0, p, 1:9] = shift_rows(block, 1, 32).astype(BF16).reshape(8, 32, 128)
        pc[2, p, 1:9] = shift_rows(block, -1, 32).astype(BF16).reshape(8, 32, 128)

    def pool_plane(q):
        even = pool[q, pl.ds(0, 256, stride=2), :]
        odd = pool[q, pl.ds(1, 256, stride=2), :]
        pc[1, q + 1, 1:9] = ((even + odd) * 0.125).astype(BF16).reshape(8, 32, 128)

    def neighbour(ref, sems, side):
        return pltpu.make_async_remote_copy(
            ref.at[2 if side == 0 else 1, pl.ds(1, 8)],
            ref.at[0 if side == 0 else 3, pl.ds(1, 8)],
            sems.at[0, side], sems.at[1, side],
            device_id=right if side == 0 else left, device_id_type=MESH,
        )

    pool[0] = fine_forward(1)
    pool[1] = fine_forward(2)
    for side in range(2):
        for e in range(2):
            halo(side, e).wait()

    @pl.when(i == 0)
    def _():
        v[1, 0, 1:9] = jnp.zeros((8, 64, 256), BF16)

    @pl.when(i == 63)
    def _():
        v[1, 5, 1:9] = jnp.zeros((8, 64, 256), BF16)

    shift_fine(0)
    shift_fine(5)
    pool[0] = pool[0] + fine_forward(0)
    pool_plane(0)
    neighbour(pc.at[1], sem_p, 1).start()
    pool[1] = pool[1] + fine_forward(3)
    pool_plane(1)
    neighbour(pc.at[1], sem_p, 0).start()
    shift_pooled(1)
    shift_pooled(2)
    load_ck.wait()
    load_ct.wait()

    def piece(q, a, b, c):
        return pc[c, q + a, b : b + 8].reshape(256, 128)

    def coarse_part(q, planes):
        taps = [(a, b, c) for a in planes for b in range(3) for c in range(3)]
        acc = None
        for at in range(0, len(taps), 2):
            some = taps[at : at + 2]
            x = jnp.concatenate([piece(q, *tap) for tap in some], axis=1)
            w = jnp.concatenate([ck[9 * a + 3 * b + c] for a, b, c in some], axis=0)
            term = mm(x, w)
            acc = term if acc is None else acc + term
        return acc

    cacc[0] = coarse_part(0, (1, 2))
    cacc[1] = coarse_part(1, (0, 1))
    for side in range(2):
        neighbour(pc.at[1], sem_p, side).wait()

    @pl.when(i == 0)
    def _():
        pc[1, 0, 1:9] = jnp.zeros((8, 32, 128), BF16)

    @pl.when(i == 63)
    def _():
        pc[1, 3, 1:9] = jnp.zeros((8, 32, 128), BF16)

    shift_pooled(0)
    shift_pooled(3)
    for q in range(2):
        pre = cacc[q] + coarse_part(q, (0,) if q == 0 else (2,))
        sig = sigmoid(pre)
        act = pre * sig
        outb[q] = act.astype(BF16).reshape(8, 32, 256)
        grad = ct[q].reshape(256, 256).astype(F32)
        cd[q + 1, 1:9] = (grad * (sig + act * (1.0 - sig))).astype(BF16).reshape(8, 32, 256)
        neighbour(cd, sem_c, 1 - q).start()
    store_out = pltpu.make_async_copy(outb, out_hbm, sem_out)
    store_out.start()

    delta = cd[1:3, 1:9].reshape(512, 256)
    for unit in coarse_units:
        lhs = mm_nt(permutation(256, unit.first, 256), delta).astype(BF16)
        for at in range(0, len(unit.taps), 2):
            some = unit.taps[at : at + 2]
            x = jnp.concatenate(
                [
                    pc[t % 3, t // 9 : t // 9 + 2, t // 3 % 3 : t // 3 % 3 + 8].reshape(512, 128)
                    for t in some
                ],
                axis=1,
            )
            term = mm(lhs, x)
            for k in range(len(some)):
                unit.put(at + k, term[:, k * 128 : (k + 1) * 128])
        unit.step_core()

    def back_part(q, planes):
        near, far = None, None
        for a in planes:
            for b in range(3):
                t = 9 * a + 3 * b
                x = cd[q + 2 - a, 2 - b : 10 - b].reshape(256, 256)
                one = mm_nt(x, ck[t : t + 2].reshape(256, 256))
                two = mm_nt(x, ck[t + 2])
                near = one if near is None else near + one
                far = two if far is None else far + two
        return near, far

    near0, far0 = back_part(0, (0, 1))
    near1, far1 = back_part(1, (1, 2))
    cacc[0], cacc[1] = near0, near1
    spr[0, 0:256], spr[1, 0:256] = far0, far1
    for side in range(2):
        neighbour(cd, sem_c, side).wait()

    @pl.when(i == 0)
    def _():
        cd[0, 1:9] = jnp.zeros((8, 32, 256), BF16)

    @pl.when(i == 63)
    def _():
        cd[3, 1:9] = jnp.zeros((8, 32, 256), BF16)

    for unit in coarse_units:
        unit.step_a()

    for q in range(2):
        near, far = back_part(q, (2,) if q == 0 else (0,))
        near, far = near + cacc[q], far + spr[q, 0:256]
        grad = near[:, 128:] + shift_rows(near[:, :128], -1, 32) + shift_rows(far, 1, 32)
        grad = grad.astype(BF16).astype(F32) * 0.125
        spr[q, pl.ds(0, 256, stride=2), :] = grad
        spr[q, pl.ds(1, 256, stride=2), :] = grad

    orders = {}
    for k, first in enumerate(("z", "y")):
        one = permutation(128, first, 128)
        orders[first] = (k, over(beside(one, zero), beside(zero, one)))
    for p in range(4):
        wide = spr[p // 2]
        d = (beside(wide, wide) * slope[p]).astype(BF16)
        for k, pick in orders.values():
            dt[k, :, p * 512 : (p + 1) * 512] = mm_nt(pick, d).astype(BF16)

    def fine_unit(unit, groups):
        k = orders[unit.first][0]
        for j, (a, c) in enumerate(groups):
            lhs = dt[k]
            here = v[c, a : a + 4, 1:9].reshape(2048, 256)
            around = beside(
                v[c, a : a + 4, 0:8, :, 128:256].reshape(2048, 128),
                v[c, a : a + 4, 2:10, :, 0:128].reshape(2048, 128),
            )
            g1 = mm(lhs, here)
            g2 = mm(lhs, around)
            unit.put(3 * j, g1[128:, :128] + g2[:128, :128])
            unit.put(3 * j + 1, g1[:128, :128] + g1[128:, 128:])
            unit.put(3 * j + 2, g1[:128, 128:] + g2[128:, 128:])
        unit.step_core()

    fine_unit(fine_units[0], FINE_UNITS[0][1])
    for unit in coarse_units:
        unit.step_b()
    fine_unit(fine_units[1], FINE_UNITS[1][1])
    fine_units[0].step_a()
    fine_unit(fine_units[2], FINE_UNITS[2][1])
    fine_units[1].step_a()
    fine_units[0].step_b()
    fine_units[2].step_a()
    for unit in coarse_units:
        unit.step_c(coarse_out)
    fine_units[1].step_b()
    fine_units[2].step_b()
    for unit in fine_units:
        unit.step_c(fine_out)
    store_out.wait()


def shards(volumes, fine_kernel, coarse_kernel, cotangent):
    vol = volumes.reshape(4, 8, 2, 64, 128)
    any_spec = pl.BlockSpec(memory_space=pl.ANY)
    vmem = pl.BlockSpec(memory_space=pltpu.VMEM)
    scratch = [
        pltpu.VMEM((3, 6, 10, 64, 256), BF16),
        pltpu.VMEM((27, 128, 128), BF16),
        pltpu.VMEM((27, 128, 256), BF16),
        pltpu.VMEM((2, 8, 32, 256), BF16),
        pltpu.VMEM((4, 512, 256), F32),
        pltpu.VMEM((2, 512, 128), F32),
        pltpu.VMEM((2, 512, 128), F32),
        pltpu.VMEM((3, 4, 10, 32, 128), BF16),
        pltpu.VMEM((4, 10, 32, 256), BF16),
        pltpu.VMEM((2, 256, 256), F32),
        pltpu.VMEM((2, 8, 32, 256), BF16),
        pltpu.VMEM((2, 256, 2048), BF16),
        pltpu.SemaphoreType.DMA((5,)),
        pltpu.SemaphoreType.DMA,
        pltpu.SemaphoreType.DMA((2, 2, 2)),
        pltpu.SemaphoreType.DMA((2, 2)),
        pltpu.SemaphoreType.DMA((2, 2)),
    ]
    for _, taps in COARSE_UNITS:
        scratch += unit_scratch(taps, 4)
    for _, groups in FINE_UNITS:
        scratch += unit_scratch(fine_taps(groups), 2)
    out, fine, coarse = pl.pallas_call(
        kernel,
        out_shape=(
            jax.ShapeDtypeStruct((2, 8, 32, 256), BF16),
            jax.ShapeDtypeStruct((2, 3456), F32),
            jax.ShapeDtypeStruct((4, 3456), F32),
        ),
        in_specs=[any_spec] * 4,
        out_specs=(any_spec, vmem, vmem),
        scratch_shapes=scratch,
        compiler_params=pltpu.CompilerParams(
            collective_id=0, has_side_effects=True, vmem_limit_bytes=60 * 2**20
        ),
        name="unet_step",
    )(vol, fine_kernel, coarse_kernel, cotangent[0])
    return out[None], fine, coarse


def solution(mesh):
    in_specs = (
        P("sample", "space", None, None, None),
        P(),
        P(),
        P("sample", "space", None, None, None),
    )
    out_specs = (P("sample", "space", None, None, None), P("space", None), P("space", None))
    return jax.shard_map(
        shards, mesh=mesh, in_specs=in_specs, out_specs=out_specs, check_vma=False
    )
```

```python
import jax
import jax.numpy as jnp
from jax import lax
from jax.experimental import pallas as pl
from jax.experimental.pallas import tpu as pltpu
from jax.sharding import PartitionSpec as P

F32 = jnp.float32
BF16 = jnp.bfloat16
MESH = pl.DeviceIdType.MESH
NT = (((1,), (1,)), ((), ()))

COARSE_UNITS = (
    ("z", True, False, tuple(range(14))),
    ("y", True, False, tuple(range(14, 27))),
)
FINE_UNITS = (
    ("z", False, False, ((0, 0), (0, 1), (0, 2), (1, 0))),
    ("y", False, False, ((1, 1), (1, 2), (2, 0))),
    ("z", False, True, ((2, 1), (2, 2))),
)


def fine_taps(groups):
    return tuple(9 * a + 3 * b + c for a, c in groups for b in range(3))


def mm(x, w):
    return jnp.dot(x, w, preferred_element_type=F32)


def mm_nt(x, w):
    return lax.dot_general(x, w, NT, preferred_element_type=F32)


def sigmoid(v):
    return 1.0 / (1.0 + jnp.exp(-v))


def up16(n):
    return -(-n // 16) * 16


def place():
    s = lax.axis_index("sample")
    i = lax.axis_index("space")
    return s, i // 32, (i // 8) % 4, (i // 2) % 4, i % 2


def device(s, xl, y, z, core):
    return (s, ((xl * 4 + y) * 4 + z) * 2 + core)


def moved(ds, dxl, dy, dz, dcore):
    s, xl, y, z, core = place()
    return device(
        (s + ds) % 2, (xl + dxl) % 2, (y + dy) % 4, (z + dz) % 4, (core + dcore) % 2
    )


def b_moves():
    return [
        (do, dxl, ds) for do in range(4) for dxl in range(2) for ds in range(2)
    ]


def permutation(rows, first, width):
    s, xl, y, z, core = place()
    m = lax.broadcasted_iota(jnp.int32, (rows, width), 0)
    o = lax.broadcasted_iota(jnp.int32, (rows, width), 1)
    r = width // 64
    group = m // r
    mxl = (group % 2 + xl) % 2
    other = (group // 2) % 4
    lead = (group // 8) % 4
    mcore = ((group // 32) % 2 + core) % 2
    if first == "z":
        mz, my = (lead + z) % 4, (other + y) % 4
    else:
        mz, my = (other + z) % 4, (lead + y) % 4
    shard = ((mxl * 4 + my) * 4 + mz) * 2 + mcore
    return (shard * r + m % r == o).astype(F32).astype(BF16)


class Unit:
    def __init__(self, first, ring, twice, taps, rows, refs):
        self.first, self.ring, self.twice, self.taps, self.rows = first, ring, twice, taps, rows
        (self.own, self.send0, self.recv0, self.senda, self.recva, self.sendb, self.recvb,
         self.sendc, self.sem0, self.sema, self.semb, self.semc) = refs
        self.half = 32 * rows
        self.chunk = 8 * rows
        self.fold = up16(len(taps) * rows)
        width = len(taps) * 128
        low = len(taps) // 2 * 128
        self.low, self.high = pl.ds(0, low), pl.ds(low, width - low)

    def put(self, j, value):
        lanes = pl.ds(j * 128, 128)
        self.own[:, lanes] = value[: self.half]
        self.send0[:, lanes] = value[self.half :].astype(BF16)

    def core_copy(self):
        return pltpu.make_async_remote_copy(
            self.send0, self.recv0, self.sem0.at[0], self.sem0.at[1],
            device_id=moved(0, 0, 0, 0, 1), device_id_type=MESH,
        )

    def lead(self, d):
        return moved(0, 0, 0, d, 0) if self.first == "z" else moved(0, 0, d, 0, 0)

    def a_copy(self, d):
        return pltpu.make_async_remote_copy(
            self.senda.at[d - 1], self.recva.at[d - 1],
            self.sema.at[0, d - 1], self.sema.at[1, d - 1],
            device_id=self.lead(d), device_id_type=MESH,
        )

    def r_copy(self, k):
        slot, lanes, d = (
            (1, self.low, 1), (1, self.high, 3), (0, self.high, 1), (2, self.low, 3),
            (0, self.low, 1), (2, self.high, 3),
        )[k]
        return pltpu.make_async_remote_copy(
            self.senda.at[slot, :, lanes], self.recva.at[slot, :, lanes],
            self.sema.at[0, k], self.sema.at[1, k],
            device_id=self.lead(d), device_id_type=MESH,
        )

    def b_copy(self, move):
        do, dxl, ds = move
        slot = (do * 4 + dxl * 2 + ds if self.twice else do * 2 + dxl) - 1
        to = moved(ds, dxl, do, 0, 0) if self.first == "z" else moved(ds, dxl, 0, do, 0)
        return pltpu.make_async_remote_copy(
            self.sendb.at[do * 2 + dxl], self.recvb.at[slot],
            self.semb.at[0, slot], self.semb.at[1, slot],
            device_id=to, device_id_type=MESH,
        )

    def c_copy(self):
        return pltpu.make_async_remote_copy(
            self.sendc.at[0], self.sendc.at[1], self.semc.at[0], self.semc.at[1],
            device_id=moved(1, 0, 0, 0, 0), device_id_type=MESH,
        )

    def b_moves(self):
        return [m for m in b_moves()[1:] if self.twice or m[2] == 0]

    def rows_of(self, d):
        return pl.ds(d * self.chunk, self.chunk)

    def step_core(self):
        self.core_copy().start()

    def step_a(self):
        self.core_copy().wait()
        total = self.own[...] + self.recv0[...].astype(F32)
        self.own[...] = total
        if self.ring:
            self.senda[1] = self.own[self.rows_of(2), :].astype(BF16)
            self.senda[0, :, self.high] = self.own[self.rows_of(1), self.high].astype(BF16)
            self.senda[2, :, self.low] = self.own[self.rows_of(3), self.low].astype(BF16)
            for k in range(4):
                self.r_copy(k).start()
        else:
            for d in (2, 1, 3):
                self.senda[d - 1] = self.own[self.rows_of(d), :].astype(BF16)
                self.a_copy(d).start()

    def step_ring(self):
        for k in range(4):
            self.r_copy(k).wait()
        one = self.own[self.rows_of(1), self.low] + self.recva[1, :, self.low].astype(F32)
        self.senda[0, :, self.low] = one.astype(BF16)
        three = self.own[self.rows_of(3), self.high] + self.recva[1, :, self.high].astype(F32)
        self.senda[2, :, self.high] = three.astype(BF16)
        for k in range(4, 6):
            self.r_copy(k).start()

    def step_b(self):
        total = self.own[self.rows_of(0), :]
        if self.ring:
            for k in range(4, 6):
                self.r_copy(k).wait()
            total = total + self.recva[0].astype(F32) + self.recva[2].astype(F32)
        else:
            for d in range(1, 4):
                self.a_copy(d).wait()
            for d in range(1, 4):
                total = total + self.recva[d - 1].astype(F32)
        r = self.rows
        for q in (4, 5, 2, 3, 6, 7, 1, 0):
            rows = total[q * r : (q + 1) * r]
            pieces = [rows[:, j * 128 : (j + 1) * 128] for j in range(len(self.taps))]
            missing = self.fold - r * len(self.taps)
            if missing:
                pieces.append(jnp.zeros((missing, 128), F32))
            self.sendb[q] = jnp.concatenate(pieces, axis=0).astype(BF16)
            for move in self.b_moves():
                if move[0] * 2 + move[1] == q:
                    self.b_copy(move).start()

    def emit(self, total, out):
        r = self.rows
        for j, tap in enumerate(self.taps):
            out[:, tap * 128 : (tap + 1) * 128] = total[j * r : (j + 1) * r]

    def step_c(self, out):
        for move in self.b_moves():
            self.b_copy(move).wait()
        total = self.sendb[0].astype(F32)
        if self.twice:
            total = total + self.recvb[0].astype(F32)
            for k in range(1, 14, 2):
                total = total + (self.recvb[k].astype(F32) + self.recvb[k + 1].astype(F32))
            self.emit(total, out)
        else:
            for k in range(7):
                total = total + self.recvb[k].astype(F32)
            self.sendc[0] = total.astype(BF16)
            self.c_copy().start()

    def step_d(self, out):
        self.c_copy().wait()
        self.emit(self.sendc[0].astype(F32) + self.sendc[1].astype(F32), out)


def unit_scratch(taps, rows):
    width, half, chunk = len(taps) * 128, 32 * rows, 8 * rows
    fold = up16(len(taps) * rows)
    return [
        pltpu.VMEM((half, width), F32),
        pltpu.VMEM((half, width), BF16),
        pltpu.VMEM((half, width), BF16),
        pltpu.VMEM((3, chunk, width), BF16),
        pltpu.VMEM((3, chunk, width), BF16),
        pltpu.VMEM((8, fold, 128), BF16),
        pltpu.VMEM((15, fold, 128), BF16),
        pltpu.VMEM((2, fold, 128), BF16),
        pltpu.SemaphoreType.DMA((2,)),
        pltpu.SemaphoreType.DMA((2, 6)),
        pltpu.SemaphoreType.DMA((2, 15)),
        pltpu.SemaphoreType.DMA((2,)),
    ]


def shift_rows(block, step, period):
    size = block.shape[0]
    row = lax.broadcasted_iota(jnp.int32, block.shape, 0) % period
    if step > 0:
        return jnp.where(row == 0, 0.0, pltpu.roll(block, 1, 0))
    return jnp.where(row == period - 1, 0.0, pltpu.roll(block, size - 1, 0))


def kernel(
    vol, fk_hbm, ck_hbm, ct_hbm,
    out_hbm, fine_out, coarse_out,
    v, fk, ck, ct, slope, pool, spr, pc, cd, cacc, outb, dt, facc, ckt, picks,
    sem_in, sem_out, sem_v, sem_p, sem_c,
    *unit_refs,
):
    s, i = lax.axis_index("sample"), lax.axis_index("space")
    left = (s, (i + 63) % 64)
    right = (s, (i + 1) % 64)
    units = []
    at = 0
    for *how, taps in COARSE_UNITS:
        units.append(Unit(*how, taps, 4, unit_refs[at : at + 12]))
        at += 12
    for *how, groups in FINE_UNITS:
        units.append(Unit(*how, fine_taps(groups), 2, unit_refs[at : at + 12]))
        at += 12
    coarse_units, fine_units = units[: len(COARSE_UNITS)], units[len(COARSE_UNITS) :]

    barrier = pltpu.get_barrier_semaphore()
    moves = {(ds, dxl, do, 0, 0) for do, dxl, ds in b_moves()}
    moves |= {(ds, dxl, 0, do, 0) for do, dxl, ds in b_moves()}
    moves.discard((0, 0, 0, 0, 0))
    moves.add((0, 0, 0, 0, 1))
    peers = [moved(*move) for move in sorted(moves)] + [left, right]
    for peer in peers:
        pl.semaphore_signal(barrier, inc=1, device_id=peer, device_id_type=MESH)

    def interior(e):
        return pltpu.make_async_copy(
            vol.at[:, :, e],
            v.at[1, pl.ds(1, 4), pl.ds(1, 8), :, pl.ds(e * 128, 128)],
            sem_in.at[e],
        )

    load_fk = pltpu.make_async_copy(fk_hbm, fk, sem_in.at[2])
    load_ck = pltpu.make_async_copy(ck_hbm, ck, sem_in.at[3])
    load_ct = pltpu.make_async_copy(ct_hbm, ct, sem_in.at[4])
    interior(0).start()
    interior(1).start()
    load_fk.start()
    load_ck.start()
    load_ct.start()

    def halo(side, e):
        return pltpu.make_async_remote_copy(
            v.at[1, 4 if side == 0 else 1, pl.ds(1, 8), :, pl.ds(e * 128, 128)],
            v.at[1, 0 if side == 0 else 5, pl.ds(1, 8), :, pl.ds(e * 128, 128)],
            sem_v.at[0, side, e], sem_v.at[1, side, e],
            device_id=right if side == 0 else left, device_id_type=MESH,
        )

    for c in range(3):
        for p in range(6):
            v[c, p, 0] = jnp.zeros((64, 256), BF16)
            v[c, p, 9] = jnp.zeros((64, 256), BF16)
        for p in range(4):
            pc[c, p, 0] = jnp.zeros((32, 128), BF16)
            pc[c, p, 9] = jnp.zeros((32, 128), BF16)
    for p in range(4):
        cd[p, 0] = jnp.zeros((32, 256), BF16)
        cd[p, 9] = jnp.zeros((32, 256), BF16)

    def shift_fine(p):
        block = v[1, p, 1:9].reshape(512, 256).astype(F32)
        v[0, p, 1:9] = shift_rows(block, 1, 64).astype(BF16).reshape(8, 64, 256)
        v[2, p, 1:9] = shift_rows(block, -1, 64).astype(BF16).reshape(8, 64, 256)

    for k, first in enumerate(("z", "y")):
        picks[k] = permutation(256, first, 256)
        pick = permutation(128, first, 128)
        none = jnp.zeros((128, 128), BF16)
        picks[2 + k, 0:128, 0:128] = pick
        picks[2 + k, 0:128, 128:256] = none
        picks[2 + k, 128:256, 0:128] = none
        picks[2 + k, 128:256, 128:256] = pick
    interior(0).wait()
    interior(1).wait()
    pl.semaphore_wait(barrier, len(peers))
    for side in range(2):
        for e in range(2):
            halo(side, e).start()
    for p in range(1, 5):
        shift_fine(p)
    load_fk.wait()

    zero = jnp.zeros((128, 128), BF16)

    def beside(a, b):
        return jnp.concatenate([a, b], axis=1)

    def over(a, b):
        return jnp.concatenate([a, b], axis=0)

    def fine_part(p, planes):
        acc = None
        for a in planes:
            for c in range(3):
                k0, k1, k2 = (fk[9 * a + 3 * b + c] for b in range(3))
                here = v[c, p + a, 1:9].reshape(512, 256)
                around = beside(
                    v[c, p + a, 0:8, :, 128:256].reshape(512, 128),
                    v[c, p + a, 2:10, :, 0:128].reshape(512, 128),
                )
                term = mm(here, over(beside(k1, k0), beside(k2, k1)))
                term = term + mm(around, over(beside(k0, zero), beside(zero, k2)))
                acc = term if acc is None else acc + term
        return acc

    def fine_forward(p, acc):
        sig = sigmoid(acc)
        act = acc * sig
        slope[p] = sig + act * (1.0 - sig)
        return act[:, :128] + act[:, 128:]

    def shift_pooled(p):
        block = pc[1, p, 1:9].reshape(256, 128).astype(F32)
        pc[0, p, 1:9] = shift_rows(block, 1, 32).astype(BF16).reshape(8, 32, 128)
        pc[2, p, 1:9] = shift_rows(block, -1, 32).astype(BF16).reshape(8, 32, 128)

    def pool_plane(q):
        even = pool[q, pl.ds(0, 256, stride=2), :]
        odd = pool[q, pl.ds(1, 256, stride=2), :]
        pc[1, q + 1, 1:9] = ((even + odd) * 0.125).astype(BF16).reshape(8, 32, 128)

    def neighbour(ref, sems, side):
        return pltpu.make_async_remote_copy(
            ref.at[2 if side == 0 else 1, pl.ds(1, 8)],
            ref.at[0 if side == 0 else 3, pl.ds(1, 8)],
            sems.at[0, side], sems.at[1, side],
            device_id=right if side == 0 else left, device_id_type=MESH,
        )

    pool[0] = fine_forward(1, fine_part(1, (0, 1, 2)))
    pool[1] = fine_forward(2, fine_part(2, (0, 1, 2)))
    facc[0] = fine_part(0, (1, 2))
    facc[1] = fine_part(3, (0, 1))
    for side in range(2):
        for e in range(2):
            halo(side, e).wait()

    @pl.when(i == 0)
    def _():
        v[1, 0, 1:9] = jnp.zeros((8, 64, 256), BF16)

    @pl.when(i == 63)
    def _():
        v[1, 5, 1:9] = jnp.zeros((8, 64, 256), BF16)

    shift_fine(0)
    shift_fine(5)
    pool[0] = pool[0] + fine_forward(0, facc[0] + fine_part(0, (0,)))
    pool_plane(0)
    neighbour(pc.at[1], sem_p, 1).start()
    pool[1] = pool[1] + fine_forward(3, facc[1] + fine_part(3, (2,)))
    pool_plane(1)
    neighbour(pc.at[1], sem_p, 0).start()
    shift_pooled(1)
    shift_pooled(2)
    load_ck.wait()
    load_ct.wait()

    def piece(q, a, b, c):
        return pc[c, q + a, b : b + 8].reshape(256, 128)

    def coarse_part(q, planes):
        taps = [(a, b, c) for a in planes for b in range(3) for c in range(3)]
        acc = None
        for at in range(0, len(taps), 2):
            some = taps[at : at + 2]
            x = jnp.concatenate([piece(q, *tap) for tap in some], axis=1)
            w = jnp.concatenate([ck[9 * a + 3 * b + c] for a, b, c in some], axis=0)
            term = mm(x, w)
            acc = term if acc is None else acc + term
        return acc

    cacc[0] = coarse_part(0, (1, 2))
    cacc[1] = coarse_part(1, (0, 1))
    for t in range(27):
        ckt[t // 3, :, t % 3 * 128 : t % 3 * 128 + 128] = ck[t].T
    for side in range(2):
        neighbour(pc.at[1], sem_p, side).wait()

    @pl.when(i == 0)
    def _():
        pc[1, 0, 1:9] = jnp.zeros((8, 32, 128), BF16)

    @pl.when(i == 63)
    def _():
        pc[1, 3, 1:9] = jnp.zeros((8, 32, 128), BF16)

    shift_pooled(0)
    shift_pooled(3)
    for q in range(2):
        pre = cacc[q] + coarse_part(q, (0,) if q == 0 else (2,))
        sig = sigmoid(pre)
        act = pre * sig
        outb[q] = act.astype(BF16).reshape(8, 32, 256)
        grad = ct[q].reshape(256, 256).astype(F32)
        cd[q + 1, 1:9] = (grad * (sig + act * (1.0 - sig))).astype(BF16).reshape(8, 32, 256)
        neighbour(cd, sem_c, 1 - q).start()
    store_out = pltpu.make_async_copy(outb, out_hbm, sem_out)
    store_out.start()

    delta = cd[1:3, 1:9].reshape(512, 256)
    for unit in coarse_units:
        lhs = mm_nt(picks[0 if unit.first == "z" else 1], delta).astype(BF16)
        for at in range(0, len(unit.taps), 2):
            some = unit.taps[at : at + 2]
            x = jnp.concatenate(
                [
                    pc[t % 3, t // 9 : t // 9 + 2, t // 3 % 3 : t // 3 % 3 + 8].reshape(512, 128)
                    for t in some
                ],
                axis=1,
            )
            term = mm(lhs, x)
            for k in range(len(some)):
                unit.put(at + k, term[:, k * 128 : (k + 1) * 128])
        unit.step_core()

    def back_part(q, planes):
        near, far = None, None
        for a in planes:
            for b in range(3):
                x = cd[q + 2 - a, 2 - b : 10 - b].reshape(256, 256)
                one = mm(x, ckt[3 * a + b, :, 0:256])
                two = mm(x, ckt[3 * a + b, :, 256:384])
                near = one if near is None else near + one
                far = two if far is None else far + two
        return near, far

    near0, far0 = back_part(0, (0, 1))
    near1, far1 = back_part(1, (1, 2))
    cacc[0], cacc[1] = near0, near1
    spr[0, 0:256], spr[1, 0:256] = far0, far1
    for side in range(2):
        neighbour(cd, sem_c, side).wait()

    @pl.when(i == 0)
    def _():
        cd[0, 1:9] = jnp.zeros((8, 32, 256), BF16)

    @pl.when(i == 63)
    def _():
        cd[3, 1:9] = jnp.zeros((8, 32, 256), BF16)

    for unit in coarse_units:
        unit.step_a()

    for q in range(2):
        near, far = back_part(q, (2,) if q == 0 else (0,))
        near, far = near + cacc[q], far + spr[q, 0:256]
        grad = near[:, 128:] + shift_rows(near[:, :128], -1, 32) + shift_rows(far, 1, 32)
        grad = grad.astype(BF16).astype(F32) * 0.125
        spr[q, pl.ds(0, 256, stride=2), :] = grad
        spr[q, pl.ds(1, 256, stride=2), :] = grad

    for p in range(4):
        wide = spr[p // 2]
        d = (beside(wide, wide) * slope[p]).astype(BF16)
        for k in range(2):
            dt[k, :, p * 512 : (p + 1) * 512] = mm_nt(picks[2 + k], d).astype(BF16)

    def fine_unit(unit, groups):
        k = 0 if unit.first == "z" else 1
        for j, (a, c) in enumerate(groups):
            lhs = dt[k]
            here = v[c, a : a + 4, 1:9].reshape(2048, 256)
            around = beside(
                v[c, a : a + 4, 0:8, :, 128:256].reshape(2048, 128),
                v[c, a : a + 4, 2:10, :, 0:128].reshape(2048, 128),
            )
            g1 = mm(lhs, here)
            g2 = mm(lhs, around)
            unit.put(3 * j, g1[128:, :128] + g2[:128, :128])
            unit.put(3 * j + 1, g1[:128, :128] + g1[128:, 128:])
            unit.put(3 * j + 2, g1[:128, 128:] + g2[128:, 128:])
        unit.step_core()

    fine_unit(fine_units[0], FINE_UNITS[0][-1])
    for unit in coarse_units:
        unit.step_ring()
    fine_unit(fine_units[1], FINE_UNITS[1][-1])
    fine_units[0].step_a()
    fine_unit(fine_units[2], FINE_UNITS[2][-1])
    fine_units[1].step_a()
    for unit in coarse_units:
        unit.step_b()
    fine_units[2].step_a()
    fine_units[0].step_b()
    fine_units[1].step_b()
    fine_units[2].step_b()
    for unit in coarse_units:
        unit.step_c(coarse_out)
    fine_units[0].step_c(fine_out)
    fine_units[1].step_c(fine_out)
    for unit in coarse_units:
        unit.step_d(coarse_out)
    fine_units[0].step_d(fine_out)
    fine_units[1].step_d(fine_out)
    fine_units[2].step_c(fine_out)
    store_out.wait()


def finish(*refs):
    ins, outs, bufs, sem = refs[:3], refs[3:6], refs[6:9], refs[9]
    reads = [pltpu.make_async_copy(ins[k], bufs[k], sem.at[0, k]) for k in range(3)]
    writes = [pltpu.make_async_copy(bufs[k], outs[k], sem.at[1, k]) for k in range(3)]
    for read in reads:
        read.start()
    for read, write in zip(reads, writes):
        read.wait()
        write.start()
    for write in writes:
        write.wait()


def shards(volumes, fine_kernel, coarse_kernel, cotangent):
    vol = volumes.reshape(4, 8, 2, 64, 128)
    any_spec = pl.BlockSpec(memory_space=pl.ANY)
    vmem = pl.BlockSpec(memory_space=pltpu.VMEM)
    scratch = [
        pltpu.VMEM((3, 6, 10, 64, 256), BF16),
        pltpu.VMEM((27, 128, 128), BF16),
        pltpu.VMEM((27, 128, 256), BF16),
        pltpu.VMEM((2, 8, 32, 256), BF16),
        pltpu.VMEM((4, 512, 256), F32),
        pltpu.VMEM((2, 512, 128), F32),
        pltpu.VMEM((2, 512, 128), F32),
        pltpu.VMEM((3, 4, 10, 32, 128), BF16),
        pltpu.VMEM((4, 10, 32, 256), BF16),
        pltpu.VMEM((2, 256, 256), F32),
        pltpu.VMEM((2, 8, 32, 256), BF16),
        pltpu.VMEM((2, 256, 2048), BF16),
        pltpu.VMEM((2, 512, 256), F32),
        pltpu.VMEM((9, 256, 384), BF16),
        pltpu.VMEM((4, 256, 256), BF16),
        pltpu.SemaphoreType.DMA((5,)),
        pltpu.SemaphoreType.DMA,
        pltpu.SemaphoreType.DMA((2, 2, 2)),
        pltpu.SemaphoreType.DMA((2, 2)),
        pltpu.SemaphoreType.DMA((2, 2)),
    ]
    for *_, taps in COARSE_UNITS:
        scratch += unit_scratch(taps, 4)
    for *_, groups in FINE_UNITS:
        scratch += unit_scratch(fine_taps(groups), 2)
    results = (
        jax.ShapeDtypeStruct((2, 8, 32, 256), BF16),
        jax.ShapeDtypeStruct((2, 3456), F32),
        jax.ShapeDtypeStruct((4, 3456), F32),
    )
    made = pl.pallas_call(
        kernel,
        out_shape=results,
        in_specs=[any_spec] * 4,
        out_specs=(any_spec, vmem, vmem),
        scratch_shapes=scratch,
        compiler_params=pltpu.CompilerParams(
            collective_id=0, has_side_effects=True, vmem_limit_bytes=60 * 2**20
        ),
        name="unet_step",
    )(vol, fine_kernel, coarse_kernel, cotangent[0])
    out, fine, coarse = pl.pallas_call(
        finish,
        out_shape=results,
        in_specs=[any_spec] * 3,
        out_specs=[any_spec] * 3,
        scratch_shapes=[pltpu.VMEM(r.shape, r.dtype) for r in results]
        + [pltpu.SemaphoreType.DMA((2, 3))],
        name="finish",
    )(*made)
    return out[None], fine, coarse


def solution(mesh):
    in_specs = (
        P("sample", "space", None, None, None),
        P(),
        P(),
        P("sample", "space", None, None, None),
    )
    out_specs = (P("sample", "space", None, None, None), P("space", None), P("space", None))
    return jax.shard_map(
        shards, mesh=mesh, in_specs=in_specs, out_specs=out_specs, check_vma=False
    )
```

```python
import jax
import jax.numpy as jnp
from jax import lax
from jax.experimental import pallas as pl
from jax.experimental.pallas import tpu as pltpu
from jax.sharding import PartitionSpec as P

F32 = jnp.float32
BF16 = jnp.bfloat16
MESH = pl.DeviceIdType.MESH
NT = (((1,), (1,)), ((), ()))

COARSE_UNITS = (
    ("z", True, False, tuple(range(14))),
    ("y", True, False, tuple(range(14, 27))),
)
FINE_UNITS = (
    ("z", False, True, ((0, 0), (0, 1), (0, 2), (1, 0))),
    ("y", False, True, ((1, 1), (1, 2), (2, 0))),
    ("z", False, True, ((2, 1), (2, 2))),
)


def fine_taps(groups):
    return tuple(9 * a + 3 * b + c for a, c in groups for b in range(3))


def mm(x, w):
    return jnp.dot(x, w, preferred_element_type=F32)


def mm_nt(x, w):
    return lax.dot_general(x, w, NT, preferred_element_type=F32)


def sigmoid(v):
    return 1.0 / (1.0 + jnp.exp(-v))


def up16(n):
    return -(-n // 16) * 16


def place():
    s = lax.axis_index("sample")
    i = lax.axis_index("space")
    return s, i // 32, (i // 8) % 4, (i // 2) % 4, i % 2


def device(s, xl, y, z, core):
    return (s, ((xl * 4 + y) * 4 + z) * 2 + core)


def moved(ds, dxl, dy, dz, dcore):
    s, xl, y, z, core = place()
    return device(
        (s + ds) % 2, (xl + dxl) % 2, (y + dy) % 4, (z + dz) % 4, (core + dcore) % 2
    )


def b_moves():
    return [
        (do, dxl, ds) for do in range(4) for dxl in range(2) for ds in range(2)
    ]


def permutation(rows, first, width):
    s, xl, y, z, core = place()
    m = lax.broadcasted_iota(jnp.int32, (rows, width), 0)
    o = lax.broadcasted_iota(jnp.int32, (rows, width), 1)
    r = width // 64
    group = m // r
    mxl = (group % 2 + xl) % 2
    other = (group // 2) % 4
    lead = (group // 8) % 4
    mcore = ((group // 32) % 2 + core) % 2
    if first == "z":
        mz, my = (lead + z) % 4, (other + y) % 4
    else:
        mz, my = (other + z) % 4, (lead + y) % 4
    shard = ((mxl * 4 + my) * 4 + mz) * 2 + mcore
    return (shard * r + m % r == o).astype(F32).astype(BF16)


class Unit:
    def __init__(self, first, ring, twice, taps, rows, refs):
        self.first, self.ring, self.twice, self.taps, self.rows = first, ring, twice, taps, rows
        (self.own, self.send0, self.recv0, self.senda, self.recva, self.sendb, self.recvb,
         self.sendc, self.sem0, self.sema, self.semb, self.semc) = refs
        self.half = 32 * rows
        self.chunk = 8 * rows
        self.fold = up16(len(taps) * rows)
        width = len(taps) * 128
        low = len(taps) // 2 * 128
        self.low, self.high = pl.ds(0, low), pl.ds(low, width - low)

    def put(self, j, value):
        lanes = pl.ds(j * 128, 128)
        self.own[:, lanes] = value[: self.half]
        self.send0[:, lanes] = value[self.half :].astype(BF16)

    def core_copy(self):
        return pltpu.make_async_remote_copy(
            self.send0, self.recv0, self.sem0.at[0], self.sem0.at[1],
            device_id=moved(0, 0, 0, 0, 1), device_id_type=MESH,
        )

    def lead(self, d):
        return moved(0, 0, 0, d, 0) if self.first == "z" else moved(0, 0, d, 0, 0)

    def a_copy(self, d):
        return pltpu.make_async_remote_copy(
            self.senda.at[d - 1], self.recva.at[d - 1],
            self.sema.at[0, d - 1], self.sema.at[1, d - 1],
            device_id=self.lead(d), device_id_type=MESH,
        )

    def r_copy(self, k):
        slot, lanes, d = (
            (1, self.low, 1), (1, self.high, 3), (0, self.high, 1), (2, self.low, 3),
            (0, self.low, 1), (2, self.high, 3),
        )[k]
        return pltpu.make_async_remote_copy(
            self.senda.at[slot, :, lanes], self.recva.at[slot, :, lanes],
            self.sema.at[0, k], self.sema.at[1, k],
            device_id=self.lead(d), device_id_type=MESH,
        )

    def b_copy(self, move):
        do, dxl, ds = move
        slot = (do * 4 + dxl * 2 + ds if self.twice else do * 2 + dxl) - 1
        to = moved(ds, dxl, do, 0, 0) if self.first == "z" else moved(ds, dxl, 0, do, 0)
        return pltpu.make_async_remote_copy(
            self.sendb.at[do * 2 + dxl], self.recvb.at[slot],
            self.semb.at[0, slot], self.semb.at[1, slot],
            device_id=to, device_id_type=MESH,
        )

    def c_copy(self):
        return pltpu.make_async_remote_copy(
            self.sendc.at[0], self.sendc.at[1], self.semc.at[0], self.semc.at[1],
            device_id=moved(1, 0, 0, 0, 0), device_id_type=MESH,
        )

    def b_moves(self):
        return [m for m in b_moves()[1:] if self.twice or m[2] == 0]

    def rows_of(self, d):
        return pl.ds(d * self.chunk, self.chunk)

    def step_core(self):
        self.core_copy().start()

    def step_a(self):
        self.core_copy().wait()
        total = self.own[...] + self.recv0[...].astype(F32)
        self.own[...] = total
        if self.ring:
            self.senda[1] = self.own[self.rows_of(2), :].astype(BF16)
            self.senda[0, :, self.high] = self.own[self.rows_of(1), self.high].astype(BF16)
            self.senda[2, :, self.low] = self.own[self.rows_of(3), self.low].astype(BF16)
            for k in range(4):
                self.r_copy(k).start()
        else:
            for d in (2, 1, 3):
                self.senda[d - 1] = self.own[self.rows_of(d), :].astype(BF16)
                self.a_copy(d).start()

    def step_ring(self):
        for k in range(4):
            self.r_copy(k).wait()
        one = self.own[self.rows_of(1), self.low] + self.recva[1, :, self.low].astype(F32)
        self.senda[0, :, self.low] = one.astype(BF16)
        three = self.own[self.rows_of(3), self.high] + self.recva[1, :, self.high].astype(F32)
        self.senda[2, :, self.high] = three.astype(BF16)
        for k in range(4, 6):
            self.r_copy(k).start()

    def step_b(self):
        total = self.own[self.rows_of(0), :]
        if self.ring:
            for k in range(4, 6):
                self.r_copy(k).wait()
            total = total + self.recva[0].astype(F32) + self.recva[2].astype(F32)
        else:
            for d in range(1, 4):
                self.a_copy(d).wait()
            for d in range(1, 4):
                total = total + self.recva[d - 1].astype(F32)
        r = self.rows
        for q in (4, 5, 2, 3, 6, 7, 1, 0):
            rows = total[q * r : (q + 1) * r]
            pieces = [rows[:, j * 128 : (j + 1) * 128] for j in range(len(self.taps))]
            missing = self.fold - r * len(self.taps)
            if missing:
                pieces.append(jnp.zeros((missing, 128), F32))
            self.sendb[q] = jnp.concatenate(pieces, axis=0).astype(BF16)
            for move in self.b_moves():
                if move[0] * 2 + move[1] == q:
                    self.b_copy(move).start()

    def emit(self, total, out):
        r = self.rows
        for j, tap in enumerate(self.taps):
            out[:, tap * 128 : (tap + 1) * 128] = total[j * r : (j + 1) * r]

    def step_c(self, out):
        for move in self.b_moves():
            self.b_copy(move).wait()
        total = self.sendb[0].astype(F32)
        if self.twice:
            total = total + self.recvb[0].astype(F32)
            for k in range(1, 14, 2):
                total = total + (self.recvb[k].astype(F32) + self.recvb[k + 1].astype(F32))
            self.emit(total, out)
        else:
            for k in range(7):
                total = total + self.recvb[k].astype(F32)
            self.sendc[0] = total.astype(BF16)
            self.c_copy().start()

    def step_d(self, out):
        self.c_copy().wait()
        self.emit(self.sendc[0].astype(F32) + self.sendc[1].astype(F32), out)


def unit_scratch(taps, rows):
    width, half, chunk = len(taps) * 128, 32 * rows, 8 * rows
    fold = up16(len(taps) * rows)
    return [
        pltpu.VMEM((half, width), F32),
        pltpu.VMEM((half, width), BF16),
        pltpu.VMEM((half, width), BF16),
        pltpu.VMEM((3, chunk, width), BF16),
        pltpu.VMEM((3, chunk, width), BF16),
        pltpu.VMEM((8, fold, 128), BF16),
        pltpu.VMEM((15, fold, 128), BF16),
        pltpu.VMEM((2, fold, 128), BF16),
        pltpu.SemaphoreType.DMA((2,)),
        pltpu.SemaphoreType.DMA((2, 6)),
        pltpu.SemaphoreType.DMA((2, 15)),
        pltpu.SemaphoreType.DMA((2,)),
    ]


def shift_rows(block, step, period):
    size = block.shape[0]
    row = lax.broadcasted_iota(jnp.int32, block.shape, 0) % period
    if step > 0:
        return jnp.where(row == 0, 0.0, pltpu.roll(block, 1, 0))
    return jnp.where(row == period - 1, 0.0, pltpu.roll(block, size - 1, 0))


def kernel(
    vol, fk_hbm, ck_hbm, ct_hbm,
    out_hbm, fine_out, coarse_out,
    v, fk, ck, ct, slope, pool, spr, pc, cd, cacc, outb, dt, facc, ckt, picks,
    sem_in, sem_out, sem_v, sem_p, sem_c,
    *unit_refs,
):
    s, i = lax.axis_index("sample"), lax.axis_index("space")
    left = (s, (i + 63) % 64)
    right = (s, (i + 1) % 64)
    units = []
    at = 0
    for *how, taps in COARSE_UNITS:
        units.append(Unit(*how, taps, 4, unit_refs[at : at + 12]))
        at += 12
    for *how, groups in FINE_UNITS:
        units.append(Unit(*how, fine_taps(groups), 2, unit_refs[at : at + 12]))
        at += 12
    coarse_units, fine_units = units[: len(COARSE_UNITS)], units[len(COARSE_UNITS) :]

    barrier = pltpu.get_barrier_semaphore()
    moves = {(ds, dxl, do, 0, 0) for do, dxl, ds in b_moves()}
    moves |= {(ds, dxl, 0, do, 0) for do, dxl, ds in b_moves()}
    moves.discard((0, 0, 0, 0, 0))
    moves.add((0, 0, 0, 0, 1))
    peers = [moved(*move) for move in sorted(moves)] + [left, right]
    for peer in peers:
        pl.semaphore_signal(barrier, inc=1, device_id=peer, device_id_type=MESH)

    def interior(e):
        return pltpu.make_async_copy(
            vol.at[:, :, e],
            v.at[1, pl.ds(1, 4), pl.ds(1, 8), :, pl.ds(e * 128, 128)],
            sem_in.at[e],
        )

    load_fk = pltpu.make_async_copy(fk_hbm, fk, sem_in.at[2])
    load_ck = pltpu.make_async_copy(ck_hbm, ck, sem_in.at[3])
    load_ct = pltpu.make_async_copy(ct_hbm, ct, sem_in.at[4])
    interior(0).start()
    interior(1).start()
    load_fk.start()
    load_ck.start()
    load_ct.start()

    def halo(side, e):
        return pltpu.make_async_remote_copy(
            v.at[1, 4 if side == 0 else 1, pl.ds(1, 8), :, pl.ds(e * 128, 128)],
            v.at[1, 0 if side == 0 else 5, pl.ds(1, 8), :, pl.ds(e * 128, 128)],
            sem_v.at[0, side, e], sem_v.at[1, side, e],
            device_id=right if side == 0 else left, device_id_type=MESH,
        )

    for c in range(3):
        for p in range(6):
            v[c, p, 0] = jnp.zeros((64, 256), BF16)
            v[c, p, 9] = jnp.zeros((64, 256), BF16)
        for p in range(4):
            pc[c, p, 0] = jnp.zeros((32, 128), BF16)
            pc[c, p, 9] = jnp.zeros((32, 128), BF16)
    for p in range(4):
        cd[p, 0] = jnp.zeros((32, 256), BF16)
        cd[p, 9] = jnp.zeros((32, 256), BF16)

    def shift_fine(p):
        block = v[1, p, 1:9].reshape(512, 256).astype(F32)
        v[0, p, 1:9] = shift_rows(block, 1, 64).astype(BF16).reshape(8, 64, 256)
        v[2, p, 1:9] = shift_rows(block, -1, 64).astype(BF16).reshape(8, 64, 256)

    for k, first in enumerate(("z", "y")):
        picks[k] = permutation(256, first, 256)
        pick = permutation(128, first, 128)
        none = jnp.zeros((128, 128), BF16)
        picks[2 + k, 0:128, 0:128] = pick
        picks[2 + k, 0:128, 128:256] = none
        picks[2 + k, 128:256, 0:128] = none
        picks[2 + k, 128:256, 128:256] = pick
    interior(0).wait()
    interior(1).wait()
    pl.semaphore_wait(barrier, len(peers))
    for side in range(2):
        for e in range(2):
            halo(side, e).start()
    for p in range(1, 5):
        shift_fine(p)
    load_fk.wait()

    zero = jnp.zeros((128, 128), BF16)

    def beside(a, b):
        return jnp.concatenate([a, b], axis=1)

    def over(a, b):
        return jnp.concatenate([a, b], axis=0)

    def fine_part(p, planes):
        acc = None
        for a in planes:
            for c in range(3):
                k0, k1, k2 = (fk[9 * a + 3 * b + c] for b in range(3))
                here = v[c, p + a, 1:9].reshape(512, 256)
                around = beside(
                    v[c, p + a, 0:8, :, 128:256].reshape(512, 128),
                    v[c, p + a, 2:10, :, 0:128].reshape(512, 128),
                )
                term = mm(here, over(beside(k1, k0), beside(k2, k1)))
                term = term + mm(around, over(beside(k0, zero), beside(zero, k2)))
                acc = term if acc is None else acc + term
        return acc

    def fine_forward(p, acc):
        sig = sigmoid(acc)
        act = acc * sig
        slope[p] = sig + act * (1.0 - sig)
        return act[:, :128] + act[:, 128:]

    def shift_pooled(p):
        block = pc[1, p, 1:9].reshape(256, 128).astype(F32)
        pc[0, p, 1:9] = shift_rows(block, 1, 32).astype(BF16).reshape(8, 32, 128)
        pc[2, p, 1:9] = shift_rows(block, -1, 32).astype(BF16).reshape(8, 32, 128)

    def pool_plane(q):
        even = pool[q, pl.ds(0, 256, stride=2), :]
        odd = pool[q, pl.ds(1, 256, stride=2), :]
        pc[1, q + 1, 1:9] = ((even + odd) * 0.125).astype(BF16).reshape(8, 32, 128)

    def neighbour(ref, sems, side):
        return pltpu.make_async_remote_copy(
            ref.at[2 if side == 0 else 1, pl.ds(1, 8)],
            ref.at[0 if side == 0 else 3, pl.ds(1, 8)],
            sems.at[0, side], sems.at[1, side],
            device_id=right if side == 0 else left, device_id_type=MESH,
        )

    pool[0] = fine_forward(1, fine_part(1, (0, 1, 2)))
    pool[1] = fine_forward(2, fine_part(2, (0, 1, 2)))
    facc[0] = fine_part(0, (1, 2))
    facc[1] = fine_part(3, (0, 1))
    for e in range(2):
        halo(0, e).wait_recv()

    @pl.when(i == 0)
    def _():
        v[1, 0, 1:9] = jnp.zeros((8, 64, 256), BF16)

    shift_fine(0)
    pool[0] = pool[0] + fine_forward(0, facc[0] + fine_part(0, (0,)))
    pool_plane(0)
    neighbour(pc.at[1], sem_p, 1).start()
    for e in range(2):
        halo(1, e).wait_recv()

    @pl.when(i == 63)
    def _():
        v[1, 5, 1:9] = jnp.zeros((8, 64, 256), BF16)

    shift_fine(5)
    pool[1] = pool[1] + fine_forward(3, facc[1] + fine_part(3, (2,)))
    pool_plane(1)
    neighbour(pc.at[1], sem_p, 0).start()
    shift_pooled(1)
    shift_pooled(2)
    load_ck.wait()
    load_ct.wait()

    def piece(q, a, b, c):
        return pc[c, q + a, b : b + 8].reshape(256, 128)

    def coarse_part(q, planes):
        taps = [(a, b, c) for a in planes for b in range(3) for c in range(3)]
        acc = None
        for at in range(0, len(taps), 2):
            some = taps[at : at + 2]
            x = jnp.concatenate([piece(q, *tap) for tap in some], axis=1)
            w = jnp.concatenate([ck[9 * a + 3 * b + c] for a, b, c in some], axis=0)
            term = mm(x, w)
            acc = term if acc is None else acc + term
        return acc

    cacc[0] = coarse_part(0, (1, 2))
    cacc[1] = coarse_part(1, (0, 1))
    for t in range(27):
        ckt[t // 3, :, t % 3 * 128 : t % 3 * 128 + 128] = ck[t].T
    def coarse_plane(q):
        neighbour(pc.at[1], sem_p, q).wait_recv()

        @pl.when(i == 63 * q)
        def _():
            pc[1, 3 * q, 1:9] = jnp.zeros((8, 32, 128), BF16)

        shift_pooled(3 * q)
        pre = cacc[q] + coarse_part(q, (0,) if q == 0 else (2,))
        sig = sigmoid(pre)
        act = pre * sig
        outb[q] = act.astype(BF16).reshape(8, 32, 256)
        grad = ct[q].reshape(256, 256).astype(F32)
        cd[q + 1, 1:9] = (grad * (sig + act * (1.0 - sig))).astype(BF16).reshape(8, 32, 256)
        neighbour(cd, sem_c, 1 - q).start()

    coarse_plane(0)
    coarse_plane(1)
    store_out = pltpu.make_async_copy(outb, out_hbm, sem_out)
    store_out.start()

    delta = cd[1:3, 1:9].reshape(512, 256)
    for unit in coarse_units:
        lhs = mm_nt(picks[0 if unit.first == "z" else 1], delta).astype(BF16)
        for at in range(0, len(unit.taps), 2):
            some = unit.taps[at : at + 2]
            x = jnp.concatenate(
                [
                    pc[t % 3, t // 9 : t // 9 + 2, t // 3 % 3 : t // 3 % 3 + 8].reshape(512, 128)
                    for t in some
                ],
                axis=1,
            )
            term = mm(lhs, x)
            for k in range(len(some)):
                unit.put(at + k, term[:, k * 128 : (k + 1) * 128])
        unit.step_core()

    def back_part(q, planes):
        near, far = None, None
        for a in planes:
            for b in range(3):
                x = cd[q + 2 - a, 2 - b : 10 - b].reshape(256, 256)
                one = mm(x, ckt[3 * a + b, :, 0:256])
                two = mm(x, ckt[3 * a + b, :, 256:384])
                near = one if near is None else near + one
                far = two if far is None else far + two
        return near, far

    near0, far0 = back_part(0, (0, 1))
    near1, far1 = back_part(1, (1, 2))
    cacc[0], cacc[1] = near0, near1
    spr[0, 0:256], spr[1, 0:256] = far0, far1
    for unit in coarse_units:
        unit.step_a()

    def fine_planes(q):
        neighbour(cd, sem_c, q).wait_recv()

        @pl.when(i == 63 * q)
        def _():
            cd[3 * q, 1:9] = jnp.zeros((8, 32, 256), BF16)

        near, far = back_part(q, (2,) if q == 0 else (0,))
        near, far = near + cacc[q], far + spr[q, 0:256]
        grad = near[:, 128:] + shift_rows(near[:, :128], -1, 32) + shift_rows(far, 1, 32)
        grad = grad.astype(BF16).astype(F32) * 0.125
        spr[q, pl.ds(0, 256, stride=2), :] = grad
        spr[q, pl.ds(1, 256, stride=2), :] = grad
        wide = spr[q]
        for p in (2 * q, 2 * q + 1):
            d = (beside(wide, wide) * slope[p]).astype(BF16)
            for k in range(2):
                dt[k, :, p * 512 : (p + 1) * 512] = mm_nt(picks[2 + k], d).astype(BF16)

    fine_planes(0)
    fine_planes(1)
    for unit in coarse_units:
        unit.step_ring()

    def before(a, c):
        return v[c, a : a + 4, 0:8, :, 128:256].reshape(2048, 128)

    def after(a, c):
        return v[c, a : a + 4, 2:10, :, 0:128].reshape(2048, 128)

    def fine_groups(unit, groups, at, count):
        k = 0 if unit.first == "z" else 1
        some = groups[at : at + count]
        if count == 2:
            low = mm(dt[k, 0:128], beside(*(before(*g) for g in some)))
            high = mm(dt[k, 128:256], beside(*(after(*g) for g in some)))
            lows = low[:, :128], low[:, 128:]
            highs = high[:, :128], high[:, 128:]
        else:
            both = mm(dt[k], beside(before(*some[0]), after(*some[0])))
            lows, highs = (both[:128, :128],), (both[128:, 128:],)
        for j, (a, c) in enumerate(some):
            mid = mm(dt[k], v[c, a : a + 4, 1:9].reshape(2048, 256))
            tap = 3 * (at + j)
            unit.put(tap, mid[128:, :128] + lows[j])
            unit.put(tap + 1, mid[:128, :128] + mid[128:, 128:])
            unit.put(tap + 2, mid[:128, 128:] + highs[j])
    one, two, three = fine_units
    groups = [unit[-1] for unit in FINE_UNITS]
    fine_groups(one, groups[0], 0, 2)
    fine_groups(one, groups[0], 2, 2)
    one.step_core()
    fine_groups(two, groups[1], 0, 2)
    one.step_a()
    fine_groups(two, groups[1], 2, 1)
    two.step_core()
    for unit in coarse_units:
        unit.step_b()
    fine_groups(three, groups[2], 0, 2)
    three.step_core()
    two.step_a()
    three.step_a()
    one.step_b()
    two.step_b()
    three.step_b()
    for unit in coarse_units:
        unit.step_c(coarse_out)
    one.step_c(fine_out)
    two.step_c(fine_out)
    for unit in coarse_units:
        unit.step_d(coarse_out)
    three.step_c(fine_out)
    for side in range(2):
        for e in range(2):
            halo(side, e).wait_send()
        neighbour(pc.at[1], sem_p, side).wait_send()
        neighbour(cd, sem_c, side).wait_send()
    store_out.wait()


def finish(*refs):
    ins, outs, bufs, sem = refs[:3], refs[3:6], refs[6:9], refs[9]
    reads = [pltpu.make_async_copy(ins[k], bufs[k], sem.at[0, k]) for k in range(3)]
    writes = [pltpu.make_async_copy(bufs[k], outs[k], sem.at[1, k]) for k in range(3)]
    for read in reads:
        read.start()
    for read, write in zip(reads, writes):
        read.wait()
        write.start()
    for write in writes:
        write.wait()


def shards(volumes, fine_kernel, coarse_kernel, cotangent):
    vol = volumes.reshape(4, 8, 2, 64, 128)
    any_spec = pl.BlockSpec(memory_space=pl.ANY)
    vmem = pl.BlockSpec(memory_space=pltpu.VMEM)
    scratch = [
        pltpu.VMEM((3, 6, 10, 64, 256), BF16),
        pltpu.VMEM((27, 128, 128), BF16),
        pltpu.VMEM((27, 128, 256), BF16),
        pltpu.VMEM((2, 8, 32, 256), BF16),
        pltpu.VMEM((4, 512, 256), F32),
        pltpu.VMEM((2, 512, 128), F32),
        pltpu.VMEM((2, 512, 128), F32),
        pltpu.VMEM((3, 4, 10, 32, 128), BF16),
        pltpu.VMEM((4, 10, 32, 256), BF16),
        pltpu.VMEM((2, 256, 256), F32),
        pltpu.VMEM((2, 8, 32, 256), BF16),
        pltpu.VMEM((2, 256, 2048), BF16),
        pltpu.VMEM((2, 512, 256), F32),
        pltpu.VMEM((9, 256, 384), BF16),
        pltpu.VMEM((4, 256, 256), BF16),
        pltpu.SemaphoreType.DMA((5,)),
        pltpu.SemaphoreType.DMA,
        pltpu.SemaphoreType.DMA((2, 2, 2)),
        pltpu.SemaphoreType.DMA((2, 2)),
        pltpu.SemaphoreType.DMA((2, 2)),
    ]
    for *_, taps in COARSE_UNITS:
        scratch += unit_scratch(taps, 4)
    for *_, groups in FINE_UNITS:
        scratch += unit_scratch(fine_taps(groups), 2)
    results = (
        jax.ShapeDtypeStruct((2, 8, 32, 256), BF16),
        jax.ShapeDtypeStruct((2, 3456), F32),
        jax.ShapeDtypeStruct((4, 3456), F32),
    )
    made = pl.pallas_call(
        kernel,
        out_shape=results,
        in_specs=[any_spec] * 4,
        out_specs=(any_spec, vmem, vmem),
        scratch_shapes=scratch,
        compiler_params=pltpu.CompilerParams(
            collective_id=0, has_side_effects=True, vmem_limit_bytes=60 * 2**20
        ),
        name="unet_step",
    )(vol, fine_kernel, coarse_kernel, cotangent[0])
    out, fine, coarse = pl.pallas_call(
        finish,
        out_shape=results,
        in_specs=[any_spec] * 3,
        out_specs=[any_spec] * 3,
        scratch_shapes=[pltpu.VMEM(r.shape, r.dtype) for r in results]
        + [pltpu.SemaphoreType.DMA((2, 3))],
        name="finish",
    )(*made)
    return out[None], fine, coarse


def solution(mesh):
    in_specs = (
        P("sample", "space", None, None, None),
        P(),
        P(),
        P("sample", "space", None, None, None),
    )
    out_specs = (P("sample", "space", None, None, None), P("space", None), P("space", None))
    return jax.shard_map(
        shards, mesh=mesh, in_specs=in_specs, out_specs=out_specs, check_vma=False
    )
```

```python
import jax
import jax.numpy as jnp
from jax import lax
from jax.experimental import pallas as pl
from jax.experimental.pallas import tpu as pltpu
from jax.sharding import PartitionSpec as P

F32 = jnp.float32
BF16 = jnp.bfloat16
MESH = pl.DeviceIdType.MESH
NT = (((1,), (1,)), ((), ()))

COARSE_UNITS = (
    ("z", True, False, tuple(range(14))),
    ("y", True, False, tuple(range(14, 27))),
)
FINE_UNITS = (
    ("z", False, True, ((0, 0), (0, 1), (0, 2), (1, 0))),
    ("y", False, True, ((1, 1), (1, 2), (2, 0))),
    ("z", False, True, ((2, 1), (2, 2))),
)


def fine_taps(groups):
    return tuple(9 * a + 3 * b + c for a, c in groups for b in range(3))


def mm(x, w):
    return jnp.dot(x, w, preferred_element_type=F32)


def mm_nt(x, w):
    return lax.dot_general(x, w, NT, preferred_element_type=F32)


def sigmoid(v):
    return 1.0 / (1.0 + jnp.exp(-v))


def up16(n):
    return -(-n // 16) * 16


def place():
    s = lax.axis_index("sample")
    i = lax.axis_index("space")
    return s, i // 32, (i // 8) % 4, (i // 2) % 4, i % 2


def device(s, xl, y, z, core):
    return (s, ((xl * 4 + y) * 4 + z) * 2 + core)


def moved(ds, dxl, dy, dz, dcore):
    s, xl, y, z, core = place()
    return device(
        (s + ds) % 2, (xl + dxl) % 2, (y + dy) % 4, (z + dz) % 4, (core + dcore) % 2
    )


def b_moves():
    return [
        (do, dxl, ds) for do in range(4) for dxl in range(2) for ds in range(2)
    ]


def permutation(rows, first, width):
    s, xl, y, z, core = place()
    m = lax.broadcasted_iota(jnp.int32, (rows, width), 0)
    o = lax.broadcasted_iota(jnp.int32, (rows, width), 1)
    r = width // 64
    group = m // r
    mxl = (group % 2 + xl) % 2
    other = (group // 2) % 4
    lead = (group // 8) % 4
    mcore = ((group // 32) % 2 + core) % 2
    if first == "z":
        mz, my = (lead + z) % 4, (other + y) % 4
    else:
        mz, my = (other + z) % 4, (lead + y) % 4
    shard = ((mxl * 4 + my) * 4 + mz) * 2 + mcore
    return (shard * r + m % r == o).astype(F32).astype(BF16)


class Unit:
    def __init__(self, first, ring, twice, taps, rows, refs):
        self.first, self.ring, self.twice, self.taps, self.rows = first, ring, twice, taps, rows
        (self.own, self.send0, self.recv0, self.senda, self.recva, self.sendb, self.recvb,
         self.sendc, self.sem0, self.sema, self.semb, self.semc) = refs
        self.half = 32 * rows
        self.chunk = 8 * rows
        self.fold = up16(len(taps) * rows)
        width = len(taps) * 128
        low = len(taps) // 2 * 128
        self.low, self.high = pl.ds(0, low), pl.ds(low, width - low)

    def put(self, j, value):
        lanes = pl.ds(j * 128, 128)
        self.own[:, lanes] = value[: self.half]
        self.send0[:, lanes] = value[self.half :].astype(BF16)

    def core_copy(self):
        return pltpu.make_async_remote_copy(
            self.send0, self.recv0, self.sem0.at[0], self.sem0.at[1],
            device_id=moved(0, 0, 0, 0, 1), device_id_type=MESH,
        )

    def lead(self, d):
        return moved(0, 0, 0, d, 0) if self.first == "z" else moved(0, 0, d, 0, 0)

    def a_copy(self, d):
        return pltpu.make_async_remote_copy(
            self.senda.at[d - 1], self.recva.at[d - 1],
            self.sema.at[0, d - 1], self.sema.at[1, d - 1],
            device_id=self.lead(d), device_id_type=MESH,
        )

    def r_copy(self, k):
        slot, lanes, d = (
            (1, self.low, 1), (1, self.high, 3), (0, self.high, 1), (2, self.low, 3),
            (0, self.low, 1), (2, self.high, 3),
        )[k]
        return pltpu.make_async_remote_copy(
            self.senda.at[slot, :, lanes], self.recva.at[slot, :, lanes],
            self.sema.at[0, k], self.sema.at[1, k],
            device_id=self.lead(d), device_id_type=MESH,
        )

    def b_copy(self, move):
        do, dxl, ds = move
        slot = (do * 4 + dxl * 2 + ds if self.twice else do * 2 + dxl) - 1
        to = moved(ds, dxl, do, 0, 0) if self.first == "z" else moved(ds, dxl, 0, do, 0)
        return pltpu.make_async_remote_copy(
            self.sendb.at[do * 2 + dxl], self.recvb.at[slot],
            self.semb.at[0, slot], self.semb.at[1, slot],
            device_id=to, device_id_type=MESH,
        )

    def c_copy(self):
        return pltpu.make_async_remote_copy(
            self.sendc.at[0], self.sendc.at[1], self.semc.at[0], self.semc.at[1],
            device_id=moved(1, 0, 0, 0, 0), device_id_type=MESH,
        )

    def b_moves(self):
        return [m for m in b_moves()[1:] if self.twice or m[2] == 0]

    def rows_of(self, d):
        return pl.ds(d * self.chunk, self.chunk)

    def step_core(self):
        self.core_copy().start()

    def step_a(self):
        self.core_copy().wait()
        total = self.own[...] + self.recv0[...].astype(F32)
        self.own[...] = total
        if self.ring:
            self.senda[1] = self.own[self.rows_of(2), :].astype(BF16)
            self.senda[0, :, self.high] = self.own[self.rows_of(1), self.high].astype(BF16)
            self.senda[2, :, self.low] = self.own[self.rows_of(3), self.low].astype(BF16)
            for k in range(4):
                self.r_copy(k).start()
        else:
            for d in (2, 1, 3):
                self.senda[d - 1] = self.own[self.rows_of(d), :].astype(BF16)
                self.a_copy(d).start()

    def step_ring(self):
        for k in range(2):
            self.r_copy(k).wait()
        one = self.own[self.rows_of(1), self.low] + self.recva[1, :, self.low].astype(F32)
        self.senda[0, :, self.low] = one.astype(BF16)
        three = self.own[self.rows_of(3), self.high] + self.recva[1, :, self.high].astype(F32)
        self.senda[2, :, self.high] = three.astype(BF16)
        for k in range(4, 6):
            self.r_copy(k).start()

    def step_b(self):
        total = self.own[self.rows_of(0), :]
        if self.ring:
            for k in range(2, 6):
                self.r_copy(k).wait()
            total = total + self.recva[0].astype(F32) + self.recva[2].astype(F32)
        else:
            for d in range(1, 4):
                self.a_copy(d).wait()
            for d in range(1, 4):
                total = total + self.recva[d - 1].astype(F32)
        r = self.rows
        for q in (4, 5, 2, 3, 6, 7, 1, 0):
            rows = total[q * r : (q + 1) * r]
            pieces = [rows[:, j * 128 : (j + 1) * 128] for j in range(len(self.taps))]
            missing = self.fold - r * len(self.taps)
            if missing:
                pieces.append(jnp.zeros((missing, 128), F32))
            self.sendb[q] = jnp.concatenate(pieces, axis=0).astype(BF16)
            for move in self.b_moves():
                if move[0] * 2 + move[1] == q:
                    self.b_copy(move).start()

    def emit(self, total, out):
        r = self.rows
        for j, tap in enumerate(self.taps):
            out[:, tap * 128 : (tap + 1) * 128] = total[j * r : (j + 1) * r]

    def step_c(self, out):
        for move in self.b_moves():
            self.b_copy(move).wait()
        total = self.sendb[0].astype(F32)
        if self.twice:
            total = total + self.recvb[0].astype(F32)
            for k in range(1, 14, 2):
                total = total + (self.recvb[k].astype(F32) + self.recvb[k + 1].astype(F32))
            self.emit(total, out)
        else:
            for k in range(7):
                total = total + self.recvb[k].astype(F32)
            self.sendc[0] = total.astype(BF16)
            self.c_copy().start()

    def step_d(self, out):
        self.c_copy().wait()
        self.emit(self.sendc[0].astype(F32) + self.sendc[1].astype(F32), out)


def unit_scratch(taps, rows):
    width, half, chunk = len(taps) * 128, 32 * rows, 8 * rows
    fold = up16(len(taps) * rows)
    return [
        pltpu.VMEM((half, width), F32),
        pltpu.VMEM((half, width), BF16),
        pltpu.VMEM((half, width), BF16),
        pltpu.VMEM((3, chunk, width), BF16),
        pltpu.VMEM((3, chunk, width), BF16),
        pltpu.VMEM((8, fold, 128), BF16),
        pltpu.VMEM((15, fold, 128), BF16),
        pltpu.VMEM((2, fold, 128), BF16),
        pltpu.SemaphoreType.DMA((2,)),
        pltpu.SemaphoreType.DMA((2, 6)),
        pltpu.SemaphoreType.DMA((2, 15)),
        pltpu.SemaphoreType.DMA((2,)),
    ]


def shift_rows(block, step, period):
    size = block.shape[0]
    row = lax.broadcasted_iota(jnp.int32, block.shape, 0) % period
    if step > 0:
        return jnp.where(row == 0, 0.0, pltpu.roll(block, 1, 0))
    return jnp.where(row == period - 1, 0.0, pltpu.roll(block, size - 1, 0))


def kernel(
    vol, fk_hbm, ck_hbm, ct_hbm,
    out_hbm, fine_out, coarse_out,
    v, fk, ck, ct, slope, pool, spr, pc, cd, cacc, outb, dt, facc, ckt, picks,
    sem_in, sem_out, sem_v, sem_p, sem_c,
    *unit_refs,
):
    s, i = lax.axis_index("sample"), lax.axis_index("space")
    left = (s, (i + 63) % 64)
    right = (s, (i + 1) % 64)
    units = []
    at = 0
    for *how, taps in COARSE_UNITS:
        units.append(Unit(*how, taps, 4, unit_refs[at : at + 12]))
        at += 12
    for *how, groups in FINE_UNITS:
        units.append(Unit(*how, fine_taps(groups), 2, unit_refs[at : at + 12]))
        at += 12
    coarse_units, fine_units = units[: len(COARSE_UNITS)], units[len(COARSE_UNITS) :]

    barrier = pltpu.get_barrier_semaphore()
    moves = {(ds, dxl, do, 0, 0) for do, dxl, ds in b_moves()}
    moves |= {(ds, dxl, 0, do, 0) for do, dxl, ds in b_moves()}
    moves.discard((0, 0, 0, 0, 0))
    moves.add((0, 0, 0, 0, 1))
    peers = [moved(*move) for move in sorted(moves)] + [left, right]
    for peer in peers:
        pl.semaphore_signal(barrier, inc=1, device_id=peer, device_id_type=MESH)

    def interior(e):
        return pltpu.make_async_copy(
            vol.at[:, :, e],
            v.at[1, pl.ds(1, 4), pl.ds(1, 8), :, pl.ds(e * 128, 128)],
            sem_in.at[e],
        )

    load_fk = pltpu.make_async_copy(fk_hbm, fk, sem_in.at[2])
    load_ck = pltpu.make_async_copy(ck_hbm, ck, sem_in.at[3])
    load_ct = pltpu.make_async_copy(ct_hbm, ct, sem_in.at[4])
    interior(0).start()
    interior(1).start()
    load_fk.start()
    load_ck.start()
    load_ct.start()

    def halo(side, e):
        return pltpu.make_async_remote_copy(
            v.at[1, 4 if side == 0 else 1, pl.ds(1, 8), :, pl.ds(e * 128, 128)],
            v.at[1, 0 if side == 0 else 5, pl.ds(1, 8), :, pl.ds(e * 128, 128)],
            sem_v.at[0, side, e], sem_v.at[1, side, e],
            device_id=right if side == 0 else left, device_id_type=MESH,
        )

    for c in range(3):
        for p in range(6):
            v[c, p, 0] = jnp.zeros((64, 256), BF16)
            v[c, p, 9] = jnp.zeros((64, 256), BF16)
        for p in range(4):
            pc[c, p, 0] = jnp.zeros((32, 128), BF16)
            pc[c, p, 9] = jnp.zeros((32, 128), BF16)
    for p in range(4):
        cd[p, 0] = jnp.zeros((32, 256), BF16)
        cd[p, 9] = jnp.zeros((32, 256), BF16)

    def shift_fine(p):
        block = v[1, p, 1:9].reshape(512, 256).astype(F32)
        v[0, p, 1:9] = shift_rows(block, 1, 64).astype(BF16).reshape(8, 64, 256)
        v[2, p, 1:9] = shift_rows(block, -1, 64).astype(BF16).reshape(8, 64, 256)

    for k, first in enumerate(("z", "y")):
        picks[k] = permutation(256, first, 256)
        pick = permutation(128, first, 128)
        none = jnp.zeros((128, 128), BF16)
        picks[2 + k, 0:128, 0:128] = pick
        picks[2 + k, 0:128, 128:256] = none
        picks[2 + k, 128:256, 0:128] = none
        picks[2 + k, 128:256, 128:256] = pick
    interior(0).wait()
    interior(1).wait()
    pl.semaphore_wait(barrier, len(peers))
    for side in range(2):
        for e in range(2):
            halo(side, e).start()
    for p in range(1, 5):
        shift_fine(p)
    load_fk.wait()

    zero = jnp.zeros((128, 128), BF16)

    def beside(a, b):
        return jnp.concatenate([a, b], axis=1)

    def over(a, b):
        return jnp.concatenate([a, b], axis=0)

    def fine_part(p, planes):
        acc = None
        for a in planes:
            for c in range(3):
                k0, k1, k2 = (fk[9 * a + 3 * b + c] for b in range(3))
                here = v[c, p + a, 1:9].reshape(512, 256)
                around = beside(
                    v[c, p + a, 0:8, :, 128:256].reshape(512, 128),
                    v[c, p + a, 2:10, :, 0:128].reshape(512, 128),
                )
                term = mm(here, over(beside(k1, k0), beside(k2, k1)))
                term = term + mm(around, over(beside(k0, zero), beside(zero, k2)))
                acc = term if acc is None else acc + term
        return acc

    def fine_forward(p, acc):
        sig = sigmoid(acc)
        act = acc * sig
        slope[p] = sig + act * (1.0 - sig)
        return act[:, :128] + act[:, 128:]

    def shift_pooled(p):
        block = pc[1, p, 1:9].reshape(256, 128).astype(F32)
        pc[0, p, 1:9] = shift_rows(block, 1, 32).astype(BF16).reshape(8, 32, 128)
        pc[2, p, 1:9] = shift_rows(block, -1, 32).astype(BF16).reshape(8, 32, 128)

    def pool_plane(q):
        even = pool[q, pl.ds(0, 256, stride=2), :]
        odd = pool[q, pl.ds(1, 256, stride=2), :]
        pc[1, q + 1, 1:9] = ((even + odd) * 0.125).astype(BF16).reshape(8, 32, 128)

    def neighbour(ref, sems, side):
        return pltpu.make_async_remote_copy(
            ref.at[2 if side == 0 else 1, pl.ds(1, 8)],
            ref.at[0 if side == 0 else 3, pl.ds(1, 8)],
            sems.at[0, side], sems.at[1, side],
            device_id=right if side == 0 else left, device_id_type=MESH,
        )

    pool[0] = fine_forward(1, fine_part(1, (0, 1, 2)))
    pool[1] = fine_forward(2, fine_part(2, (0, 1, 2)))
    facc[0] = fine_part(0, (1, 2))
    facc[1] = fine_part(3, (0, 1))
    for e in range(2):
        halo(0, e).wait_recv()

    @pl.when(i == 0)
    def _():
        v[1, 0, 1:9] = jnp.zeros((8, 64, 256), BF16)

    shift_fine(0)
    pool[0] = pool[0] + fine_forward(0, facc[0] + fine_part(0, (0,)))
    pool_plane(0)
    neighbour(pc.at[1], sem_p, 1).start()
    for e in range(2):
        halo(1, e).wait_recv()

    @pl.when(i == 63)
    def _():
        v[1, 5, 1:9] = jnp.zeros((8, 64, 256), BF16)

    shift_fine(5)
    pool[1] = pool[1] + fine_forward(3, facc[1] + fine_part(3, (2,)))
    pool_plane(1)
    neighbour(pc.at[1], sem_p, 0).start()
    shift_pooled(1)
    shift_pooled(2)
    load_ck.wait()
    load_ct.wait()

    def piece(q, a, b, c):
        return pc[c, q + a, b : b + 8].reshape(256, 128)

    def coarse_part(q, planes):
        taps = [(a, b, c) for a in planes for b in range(3) for c in range(3)]
        acc = None
        for at in range(0, len(taps), 2):
            some = taps[at : at + 2]
            x = jnp.concatenate([piece(q, *tap) for tap in some], axis=1)
            w = jnp.concatenate([ck[9 * a + 3 * b + c] for a, b, c in some], axis=0)
            term = mm(x, w)
            acc = term if acc is None else acc + term
        return acc

    cacc[0] = coarse_part(0, (1, 2))
    cacc[1] = coarse_part(1, (0, 1))
    for t in range(27):
        ckt[t // 3, :, t % 3 * 128 : t % 3 * 128 + 128] = ck[t].T
    def coarse_plane(q):
        neighbour(pc.at[1], sem_p, q).wait_recv()

        @pl.when(i == 63 * q)
        def _():
            pc[1, 3 * q, 1:9] = jnp.zeros((8, 32, 128), BF16)

        shift_pooled(3 * q)
        pre = cacc[q] + coarse_part(q, (0,) if q == 0 else (2,))
        sig = sigmoid(pre)
        act = pre * sig
        outb[q] = act.astype(BF16).reshape(8, 32, 256)
        grad = ct[q].reshape(256, 256).astype(F32)
        cd[q + 1, 1:9] = (grad * (sig + act * (1.0 - sig))).astype(BF16).reshape(8, 32, 256)
        neighbour(cd, sem_c, 1 - q).start()

    coarse_plane(0)
    coarse_plane(1)
    store_out = pltpu.make_async_copy(outb, out_hbm, sem_out)
    store_out.start()

    delta = cd[1:3, 1:9].reshape(512, 256)
    for unit in coarse_units:
        lhs = mm_nt(picks[0 if unit.first == "z" else 1], delta).astype(BF16)
        for at in range(0, len(unit.taps), 2):
            some = unit.taps[at : at + 2]
            x = jnp.concatenate(
                [
                    pc[t % 3, t // 9 : t // 9 + 2, t // 3 % 3 : t // 3 % 3 + 8].reshape(512, 128)
                    for t in some
                ],
                axis=1,
            )
            term = mm(lhs, x)
            for k in range(len(some)):
                unit.put(at + k, term[:, k * 128 : (k + 1) * 128])
        unit.step_core()

    def back_part(q, planes):
        near, far = None, None
        for a in planes:
            for b in range(3):
                x = cd[q + 2 - a, 2 - b : 10 - b].reshape(256, 256)
                one = mm(x, ckt[3 * a + b, :, 0:256])
                two = mm(x, ckt[3 * a + b, :, 256:384])
                near = one if near is None else near + one
                far = two if far is None else far + two
        return near, far

    near0, far0 = back_part(0, (0, 1))
    near1, far1 = back_part(1, (1, 2))
    cacc[0], cacc[1] = near0, near1
    spr[0, 0:256], spr[1, 0:256] = far0, far1
    for unit in coarse_units:
        unit.step_a()

    def fine_planes(q):
        neighbour(cd, sem_c, q).wait_recv()

        @pl.when(i == 63 * q)
        def _():
            cd[3 * q, 1:9] = jnp.zeros((8, 32, 256), BF16)

        near, far = back_part(q, (2,) if q == 0 else (0,))
        near, far = near + cacc[q], far + spr[q, 0:256]
        grad = near[:, 128:] + shift_rows(near[:, :128], -1, 32) + shift_rows(far, 1, 32)
        grad = grad.astype(BF16).astype(F32) * 0.125
        spr[q, pl.ds(0, 256, stride=2), :] = grad
        spr[q, pl.ds(1, 256, stride=2), :] = grad
        wide = spr[q]
        for p in (2 * q, 2 * q + 1):
            d = (beside(wide, wide) * slope[p]).astype(BF16)
            for k in range(2):
                dt[k, :, p * 512 : (p + 1) * 512] = mm_nt(picks[2 + k], d).astype(BF16)

    fine_planes(0)
    fine_planes(1)

    def before(a, c):
        return v[c, a : a + 4, 0:8, :, 128:256].reshape(2048, 128)

    def after(a, c):
        return v[c, a : a + 4, 2:10, :, 0:128].reshape(2048, 128)

    def fine_groups(unit, groups, at, count):
        k = 0 if unit.first == "z" else 1
        some = groups[at : at + count]
        if count == 2:
            low = mm(dt[k, 0:128], beside(*(before(*g) for g in some)))
            high = mm(dt[k, 128:256], beside(*(after(*g) for g in some)))
            lows = low[:, :128], low[:, 128:]
            highs = high[:, :128], high[:, 128:]
        else:
            both = mm(dt[k], beside(before(*some[0]), after(*some[0])))
            lows, highs = (both[:128, :128],), (both[128:, 128:],)
        for j, (a, c) in enumerate(some):
            mid = mm(dt[k], v[c, a : a + 4, 1:9].reshape(2048, 256))
            tap = 3 * (at + j)
            unit.put(tap, mid[128:, :128] + lows[j])
            unit.put(tap + 1, mid[:128, :128] + mid[128:, 128:])
            unit.put(tap + 2, mid[:128, 128:] + highs[j])
    one, two, three = fine_units
    groups = [unit[-1] for unit in FINE_UNITS]
    fine_groups(one, groups[0], 0, 2)
    fine_groups(one, groups[0], 2, 2)
    one.step_core()
    for unit in coarse_units:
        unit.step_ring()
    fine_groups(two, groups[1], 0, 2)
    one.step_a()
    fine_groups(two, groups[1], 2, 1)
    two.step_core()
    fine_groups(three, groups[2], 0, 2)
    three.step_core()
    two.step_a()
    three.step_a()
    for unit in coarse_units:
        unit.step_b()
    one.step_b()
    two.step_b()
    three.step_b()
    for unit in coarse_units:
        unit.step_c(coarse_out)
    one.step_c(fine_out)
    two.step_c(fine_out)
    for unit in coarse_units:
        unit.step_d(coarse_out)
    three.step_c(fine_out)
    for side in range(2):
        for e in range(2):
            halo(side, e).wait_send()
        neighbour(pc.at[1], sem_p, side).wait_send()
        neighbour(cd, sem_c, side).wait_send()
    store_out.wait()


def finish(*refs):
    ins, outs, bufs, sem = refs[:3], refs[3:6], refs[6:9], refs[9]
    reads = [pltpu.make_async_copy(ins[k], bufs[k], sem.at[0, k]) for k in range(3)]
    writes = [pltpu.make_async_copy(bufs[k], outs[k], sem.at[1, k]) for k in range(3)]
    for read in reads:
        read.start()
    for read, write in zip(reads, writes):
        read.wait()
        write.start()
    for write in writes:
        write.wait()


def shards(volumes, fine_kernel, coarse_kernel, cotangent):
    vol = volumes.reshape(4, 8, 2, 64, 128)
    any_spec = pl.BlockSpec(memory_space=pl.ANY)
    vmem = pl.BlockSpec(memory_space=pltpu.VMEM)
    scratch = [
        pltpu.VMEM((3, 6, 10, 64, 256), BF16),
        pltpu.VMEM((27, 128, 128), BF16),
        pltpu.VMEM((27, 128, 256), BF16),
        pltpu.VMEM((2, 8, 32, 256), BF16),
        pltpu.VMEM((4, 512, 256), F32),
        pltpu.VMEM((2, 512, 128), F32),
        pltpu.VMEM((2, 512, 128), F32),
        pltpu.VMEM((3, 4, 10, 32, 128), BF16),
        pltpu.VMEM((4, 10, 32, 256), BF16),
        pltpu.VMEM((2, 256, 256), F32),
        pltpu.VMEM((2, 8, 32, 256), BF16),
        pltpu.VMEM((2, 256, 2048), BF16),
        pltpu.VMEM((2, 512, 256), F32),
        pltpu.VMEM((9, 256, 384), BF16),
        pltpu.VMEM((4, 256, 256), BF16),
        pltpu.SemaphoreType.DMA((5,)),
        pltpu.SemaphoreType.DMA,
        pltpu.SemaphoreType.DMA((2, 2, 2)),
        pltpu.SemaphoreType.DMA((2, 2)),
        pltpu.SemaphoreType.DMA((2, 2)),
    ]
    for *_, taps in COARSE_UNITS:
        scratch += unit_scratch(taps, 4)
    for *_, groups in FINE_UNITS:
        scratch += unit_scratch(fine_taps(groups), 2)
    results = (
        jax.ShapeDtypeStruct((2, 8, 32, 256), BF16),
        jax.ShapeDtypeStruct((2, 3456), F32),
        jax.ShapeDtypeStruct((4, 3456), F32),
    )
    made = pl.pallas_call(
        kernel,
        out_shape=results,
        in_specs=[any_spec] * 4,
        out_specs=(any_spec, vmem, vmem),
        scratch_shapes=scratch,
        compiler_params=pltpu.CompilerParams(
            collective_id=0, has_side_effects=True, vmem_limit_bytes=60 * 2**20
        ),
        name="unet_step",
    )(vol, fine_kernel, coarse_kernel, cotangent[0])
    out, fine, coarse = pl.pallas_call(
        finish,
        out_shape=results,
        in_specs=[any_spec] * 3,
        out_specs=[any_spec] * 3,
        scratch_shapes=[pltpu.VMEM(r.shape, r.dtype) for r in results]
        + [pltpu.SemaphoreType.DMA((2, 3))],
        name="finish",
    )(*made)
    return out[None], fine, coarse


def solution(mesh):
    in_specs = (
        P("sample", "space", None, None, None),
        P(),
        P(),
        P("sample", "space", None, None, None),
    )
    out_specs = (P("sample", "space", None, None, None), P("space", None), P("space", None))
    return jax.shard_map(
        shards, mesh=mesh, in_specs=in_specs, out_specs=out_specs, check_vma=False
    )
```

```python
import jax
import jax.numpy as jnp
from jax import lax
from jax.experimental import pallas as pl
from jax.experimental.pallas import tpu as pltpu
from jax.sharding import PartitionSpec as P

F32 = jnp.float32
BF16 = jnp.bfloat16
MESH = pl.DeviceIdType.MESH
NT = (((1,), (1,)), ((), ()))

COARSE_UNITS = (
    ("z", True, False, tuple(range(14))),
    ("y", True, False, tuple(range(14, 27))),
)
FINE_UNITS = (
    ("z", False, False, ((0, 0), (0, 1), (0, 2), (1, 0))),
    ("y", False, True, ((1, 1), (1, 2), (2, 0))),
    ("z", False, True, ((2, 1), (2, 2))),
)


def fine_taps(groups):
    return tuple(9 * a + 3 * b + c for a, c in groups for b in range(3))


def mm(x, w):
    return jnp.dot(x, w, preferred_element_type=F32)


def mm_nt(x, w):
    return lax.dot_general(x, w, NT, preferred_element_type=F32)


def sigmoid(v):
    return 1.0 / (1.0 + jnp.exp(-v))


def up16(n):
    return -(-n // 16) * 16


def place():
    s = lax.axis_index("sample")
    i = lax.axis_index("space")
    return s, i // 32, (i // 8) % 4, (i // 2) % 4, i % 2


def device(s, xl, y, z, core):
    return (s, ((xl * 4 + y) * 4 + z) * 2 + core)


def moved(ds, dxl, dy, dz, dcore):
    s, xl, y, z, core = place()
    return device(
        (s + ds) % 2, (xl + dxl) % 2, (y + dy) % 4, (z + dz) % 4, (core + dcore) % 2
    )


def b_moves():
    return [
        (do, dxl, ds) for do in range(4) for dxl in range(2) for ds in range(2)
    ]


def permutation(rows, first, width):
    s, xl, y, z, core = place()
    m = lax.broadcasted_iota(jnp.int32, (rows, width), 0)
    o = lax.broadcasted_iota(jnp.int32, (rows, width), 1)
    r = width // 64
    group = m // r
    mxl = (group % 2 + xl) % 2
    other = (group // 2) % 4
    lead = (group // 8) % 4
    mcore = ((group // 32) % 2 + core) % 2
    if first == "z":
        mz, my = (lead + z) % 4, (other + y) % 4
    else:
        mz, my = (other + z) % 4, (lead + y) % 4
    shard = ((mxl * 4 + my) * 4 + mz) * 2 + mcore
    return (shard * r + m % r == o).astype(F32).astype(BF16)


class Unit:
    def __init__(self, first, ring, twice, taps, rows, refs):
        self.first, self.ring, self.twice, self.taps, self.rows = first, ring, twice, taps, rows
        (self.own, self.send0, self.recv0, self.senda, self.recva, self.sendb, self.recvb,
         self.sendc, self.sem0, self.sema, self.semb, self.semc) = refs
        self.half = 32 * rows
        self.chunk = 8 * rows
        self.fold = up16(len(taps) * rows)
        width = len(taps) * 128
        low = len(taps) // 2 * 128
        self.low, self.high = pl.ds(0, low), pl.ds(low, width - low)

    def put(self, j, value):
        lanes = pl.ds(j * 128, 128)
        self.own[:, lanes] = value[: self.half]
        self.send0[:, lanes] = value[self.half :].astype(BF16)

    def core_copy(self):
        return pltpu.make_async_remote_copy(
            self.send0, self.recv0, self.sem0.at[0], self.sem0.at[1],
            device_id=moved(0, 0, 0, 0, 1), device_id_type=MESH,
        )

    def lead(self, d):
        return moved(0, 0, 0, d, 0) if self.first == "z" else moved(0, 0, d, 0, 0)

    def a_copy(self, d):
        return pltpu.make_async_remote_copy(
            self.senda.at[d - 1], self.recva.at[d - 1],
            self.sema.at[0, d - 1], self.sema.at[1, d - 1],
            device_id=self.lead(d), device_id_type=MESH,
        )

    def r_copy(self, k):
        slot, lanes, d = (
            (1, self.low, 1), (1, self.high, 3), (0, self.high, 1), (2, self.low, 3),
            (0, self.low, 1), (2, self.high, 3),
        )[k]
        return pltpu.make_async_remote_copy(
            self.senda.at[slot, :, lanes], self.recva.at[slot, :, lanes],
            self.sema.at[0, k], self.sema.at[1, k],
            device_id=self.lead(d), device_id_type=MESH,
        )

    def b_copy(self, move):
        do, dxl, ds = move
        slot = (do * 4 + dxl * 2 + ds if self.twice else do * 2 + dxl) - 1
        to = moved(ds, dxl, do, 0, 0) if self.first == "z" else moved(ds, dxl, 0, do, 0)
        return pltpu.make_async_remote_copy(
            self.sendb.at[do * 2 + dxl], self.recvb.at[slot],
            self.semb.at[0, slot], self.semb.at[1, slot],
            device_id=to, device_id_type=MESH,
        )

    def c_copy(self):
        return pltpu.make_async_remote_copy(
            self.sendc.at[0], self.sendc.at[1], self.semc.at[0], self.semc.at[1],
            device_id=moved(1, 0, 0, 0, 0), device_id_type=MESH,
        )

    def b_moves(self):
        return [m for m in b_moves()[1:] if self.twice or m[2] == 0]

    def rows_of(self, d):
        return pl.ds(d * self.chunk, self.chunk)

    def step_core(self):
        self.core_copy().start()

    def step_a(self):
        self.core_copy().wait()
        if not self.ring:
            for d in (2, 1, 3):
                self.senda[d - 1] = self.summed(d).astype(BF16)
                self.a_copy(d).start()
            self.own[self.rows_of(0), :] = self.summed(0)
            return
        self.senda[1] = self.summed(2).astype(BF16)
        for k in range(2):
            self.r_copy(k).start()
        for d in (1, 3, 0):
            self.own[self.rows_of(d), :] = self.summed(d)
        self.senda[0, :, self.high] = self.own[self.rows_of(1), self.high].astype(BF16)
        self.senda[2, :, self.low] = self.own[self.rows_of(3), self.low].astype(BF16)
        for k in range(2, 4):
            self.r_copy(k).start()

    def summed(self, d):
        rows = self.rows_of(d)
        return self.own[rows, :] + self.recv0[rows, :].astype(F32)

    def step_ring(self):
        for k in range(2):
            self.r_copy(k).wait()
        one = self.own[self.rows_of(1), self.low] + self.recva[1, :, self.low].astype(F32)
        self.senda[0, :, self.low] = one.astype(BF16)
        three = self.own[self.rows_of(3), self.high] + self.recva[1, :, self.high].astype(F32)
        self.senda[2, :, self.high] = three.astype(BF16)
        for k in range(4, 6):
            self.r_copy(k).start()

    def step_b(self):
        total = self.own[self.rows_of(0), :]
        if self.ring:
            for k in range(2, 6):
                self.r_copy(k).wait()
            total = total + self.recva[0].astype(F32) + self.recva[2].astype(F32)
        else:
            for d in range(1, 4):
                self.a_copy(d).wait()
            for d in range(1, 4):
                total = total + self.recva[d - 1].astype(F32)
        r = self.rows
        for q in (4, 5, 2, 3, 6, 7, 1, 0):
            rows = total[q * r : (q + 1) * r]
            pieces = [rows[:, j * 128 : (j + 1) * 128] for j in range(len(self.taps))]
            missing = self.fold - r * len(self.taps)
            if missing:
                pieces.append(jnp.zeros((missing, 128), F32))
            self.sendb[q] = jnp.concatenate(pieces, axis=0).astype(BF16)
            for move in self.b_moves():
                if move[0] * 2 + move[1] == q:
                    self.b_copy(move).start()

    def emit(self, total, out):
        r = self.rows
        for j, tap in enumerate(self.taps):
            out[:, tap * 128 : (tap + 1) * 128] = total[j * r : (j + 1) * r]

    def step_c(self, out):
        for move in self.b_moves():
            self.b_copy(move).wait()
        total = self.sendb[0].astype(F32)
        if self.twice:
            total = total + self.recvb[0].astype(F32)
            for k in range(1, 14, 2):
                total = total + (self.recvb[k].astype(F32) + self.recvb[k + 1].astype(F32))
            self.emit(total, out)
        else:
            for k in range(7):
                total = total + self.recvb[k].astype(F32)
            self.sendc[0] = total.astype(BF16)
            self.c_copy().start()

    def step_d(self, out):
        self.c_copy().wait()
        self.emit(self.sendc[0].astype(F32) + self.sendc[1].astype(F32), out)


def unit_scratch(taps, rows):
    width, half, chunk = len(taps) * 128, 32 * rows, 8 * rows
    fold = up16(len(taps) * rows)
    return [
        pltpu.VMEM((half, width), F32),
        pltpu.VMEM((half, width), BF16),
        pltpu.VMEM((half, width), BF16),
        pltpu.VMEM((3, chunk, width), BF16),
        pltpu.VMEM((3, chunk, width), BF16),
        pltpu.VMEM((8, fold, 128), BF16),
        pltpu.VMEM((15, fold, 128), BF16),
        pltpu.VMEM((2, fold, 128), BF16),
        pltpu.SemaphoreType.DMA((2,)),
        pltpu.SemaphoreType.DMA((2, 6)),
        pltpu.SemaphoreType.DMA((2, 15)),
        pltpu.SemaphoreType.DMA((2,)),
    ]


def shift_rows(block, step, period):
    size = block.shape[0]
    row = lax.broadcasted_iota(jnp.int32, block.shape, 0) % period
    if step > 0:
        return jnp.where(row == 0, 0.0, pltpu.roll(block, 1, 0))
    return jnp.where(row == period - 1, 0.0, pltpu.roll(block, size - 1, 0))


def kernel(
    vol, fk_hbm, ck_hbm, ct_hbm,
    out_hbm, fine_out, coarse_out,
    v, fk, ck, ct, slope, pool, spr, pc, cd, cacc, outb, dt, facc, ckt, picks,
    sem_in, sem_out, sem_v, sem_p, sem_c,
    *unit_refs,
):
    s, i = lax.axis_index("sample"), lax.axis_index("space")
    left = (s, (i + 63) % 64)
    right = (s, (i + 1) % 64)
    units = []
    at = 0
    for *how, taps in COARSE_UNITS:
        units.append(Unit(*how, taps, 4, unit_refs[at : at + 12]))
        at += 12
    for *how, groups in FINE_UNITS:
        units.append(Unit(*how, fine_taps(groups), 2, unit_refs[at : at + 12]))
        at += 12
    coarse_units, fine_units = units[: len(COARSE_UNITS)], units[len(COARSE_UNITS) :]

    barrier = pltpu.get_barrier_semaphore()
    moves = {(ds, dxl, do, 0, 0) for do, dxl, ds in b_moves()}
    moves |= {(ds, dxl, 0, do, 0) for do, dxl, ds in b_moves()}
    moves.discard((0, 0, 0, 0, 0))
    moves.add((0, 0, 0, 0, 1))
    peers = [left, right] + [moved(*move) for move in sorted(moves)]
    for peer in peers[:2]:
        pl.semaphore_signal(barrier, inc=1, device_id=peer, device_id_type=MESH)

    def interior(e):
        return pltpu.make_async_copy(
            vol.at[:, :, e],
            v.at[1, pl.ds(1, 4), pl.ds(1, 8), :, pl.ds(e * 128, 128)],
            sem_in.at[e],
        )

    load_fk = pltpu.make_async_copy(fk_hbm, fk, sem_in.at[2])
    load_ck = pltpu.make_async_copy(ck_hbm, ck, sem_in.at[3])
    load_ct = pltpu.make_async_copy(ct_hbm, ct, sem_in.at[4])
    interior(0).start()
    interior(1).start()
    load_fk.start()
    load_ck.start()
    load_ct.start()
    for peer in peers[2:]:
        pl.semaphore_signal(barrier, inc=1, device_id=peer, device_id_type=MESH)

    def halo(side, e):
        return pltpu.make_async_remote_copy(
            v.at[1, 4 if side == 0 else 1, pl.ds(1, 8), :, pl.ds(e * 128, 128)],
            v.at[1, 0 if side == 0 else 5, pl.ds(1, 8), :, pl.ds(e * 128, 128)],
            sem_v.at[0, side, e], sem_v.at[1, side, e],
            device_id=right if side == 0 else left, device_id_type=MESH,
        )

    for c in range(3):
        for p in range(6):
            v[c, p, 0] = jnp.zeros((64, 256), BF16)
            v[c, p, 9] = jnp.zeros((64, 256), BF16)
        for p in range(4):
            pc[c, p, 0] = jnp.zeros((32, 128), BF16)
            pc[c, p, 9] = jnp.zeros((32, 128), BF16)
    for p in range(4):
        cd[p, 0] = jnp.zeros((32, 256), BF16)
        cd[p, 9] = jnp.zeros((32, 256), BF16)

    def shift_fine(p):
        block = v[1, p, 1:9].reshape(512, 256).astype(F32)
        v[0, p, 1:9] = shift_rows(block, 1, 64).astype(BF16).reshape(8, 64, 256)
        v[2, p, 1:9] = shift_rows(block, -1, 64).astype(BF16).reshape(8, 64, 256)

    for k, first in enumerate(("z", "y")):
        picks[k] = permutation(256, first, 256)
        pick = permutation(128, first, 128)
        none = jnp.zeros((128, 128), BF16)
        picks[2 + k, 0:128, 0:128] = pick
        picks[2 + k, 0:128, 128:256] = none
        picks[2 + k, 128:256, 0:128] = none
        picks[2 + k, 128:256, 128:256] = pick
    interior(0).wait()
    interior(1).wait()
    pl.semaphore_wait(barrier, len(peers))
    for side in range(2):
        for e in range(2):
            halo(side, e).start()
    for p in range(1, 5):
        shift_fine(p)
    load_fk.wait()

    zero = jnp.zeros((128, 128), BF16)

    def beside(a, b):
        return jnp.concatenate([a, b], axis=1)

    def over(a, b):
        return jnp.concatenate([a, b], axis=0)

    def fine_part(p, planes):
        acc = None
        for a in planes:
            for c in range(3):
                k0, k1, k2 = (fk[9 * a + 3 * b + c] for b in range(3))
                here = v[c, p + a, 1:9].reshape(512, 256)
                around = beside(
                    v[c, p + a, 0:8, :, 128:256].reshape(512, 128),
                    v[c, p + a, 2:10, :, 0:128].reshape(512, 128),
                )
                term = mm(here, over(beside(k1, k0), beside(k2, k1)))
                term = term + mm(around, over(beside(k0, zero), beside(zero, k2)))
                acc = term if acc is None else acc + term
        return acc

    def fine_forward(p, acc):
        sig = sigmoid(acc)
        act = acc * sig
        slope[p] = sig + act * (1.0 - sig)
        return act[:, :128] + act[:, 128:]

    def shift_pooled(p):
        block = pc[1, p, 1:9].reshape(256, 128).astype(F32)
        pc[0, p, 1:9] = shift_rows(block, 1, 32).astype(BF16).reshape(8, 32, 128)
        pc[2, p, 1:9] = shift_rows(block, -1, 32).astype(BF16).reshape(8, 32, 128)

    def pool_plane(q):
        even = pool[q, pl.ds(0, 256, stride=2), :]
        odd = pool[q, pl.ds(1, 256, stride=2), :]
        pc[1, q + 1, 1:9] = ((even + odd) * 0.125).astype(BF16).reshape(8, 32, 128)

    def neighbour(ref, sems, side):
        return pltpu.make_async_remote_copy(
            ref.at[2 if side == 0 else 1, pl.ds(1, 8)],
            ref.at[0 if side == 0 else 3, pl.ds(1, 8)],
            sems.at[0, side], sems.at[1, side],
            device_id=right if side == 0 else left, device_id_type=MESH,
        )

    pool[0] = fine_forward(1, fine_part(1, (0, 1, 2)))
    pool[1] = fine_forward(2, fine_part(2, (0, 1, 2)))
    facc[0] = fine_part(0, (1, 2))
    facc[1] = fine_part(3, (0, 1))
    for e in range(2):
        halo(0, e).wait_recv()

    @pl.when(i == 0)
    def _():
        v[1, 0, 1:9] = jnp.zeros((8, 64, 256), BF16)

    shift_fine(0)
    pool[0] = pool[0] + fine_forward(0, facc[0] + fine_part(0, (0,)))
    pool_plane(0)
    neighbour(pc.at[1], sem_p, 1).start()
    for e in range(2):
        halo(1, e).wait_recv()

    @pl.when(i == 63)
    def _():
        v[1, 5, 1:9] = jnp.zeros((8, 64, 256), BF16)

    shift_fine(5)
    pool[1] = pool[1] + fine_forward(3, facc[1] + fine_part(3, (2,)))
    pool_plane(1)
    neighbour(pc.at[1], sem_p, 0).start()
    shift_pooled(1)
    shift_pooled(2)
    load_ck.wait()
    load_ct.wait()

    def piece(q, a, b, c):
        return pc[c, q + a, b : b + 8].reshape(256, 128)

    def coarse_part(q, planes):
        taps = [(a, b, c) for a in planes for b in range(3) for c in range(3)]
        acc = None
        for at in range(0, len(taps), 2):
            some = taps[at : at + 2]
            x = jnp.concatenate([piece(q, *tap) for tap in some], axis=1)
            w = jnp.concatenate([ck[9 * a + 3 * b + c] for a, b, c in some], axis=0)
            term = mm(x, w)
            acc = term if acc is None else acc + term
        return acc

    cacc[0] = coarse_part(0, (1, 2))
    cacc[1] = coarse_part(1, (0, 1))
    for t in range(27):
        ckt[t // 3, :, t % 3 * 128 : t % 3 * 128 + 128] = ck[t].T
    def coarse_plane(q):
        neighbour(pc.at[1], sem_p, q).wait_recv()

        @pl.when(i == 63 * q)
        def _():
            pc[1, 3 * q, 1:9] = jnp.zeros((8, 32, 128), BF16)

        shift_pooled(3 * q)
        pre = cacc[q] + coarse_part(q, (0,) if q == 0 else (2,))
        sig = sigmoid(pre)
        act = pre * sig
        outb[q] = act.astype(BF16).reshape(8, 32, 256)
        grad = ct[q].reshape(256, 256).astype(F32)
        cd[q + 1, 1:9] = (grad * (sig + act * (1.0 - sig))).astype(BF16).reshape(8, 32, 256)
        neighbour(cd, sem_c, 1 - q).start()

    coarse_plane(0)
    coarse_plane(1)
    store_out = pltpu.make_async_copy(outb, out_hbm, sem_out)
    store_out.start()

    delta = cd[1:3, 1:9].reshape(512, 256)
    orders = {
        first: mm_nt(picks[k], delta).astype(BF16) for k, first in enumerate(("z", "y"))
    }
    for unit in coarse_units:
        lhs = orders[unit.first]
        for at in range(0, len(unit.taps), 2):
            some = unit.taps[at : at + 2]
            x = jnp.concatenate(
                [
                    pc[t % 3, t // 9 : t // 9 + 2, t // 3 % 3 : t // 3 % 3 + 8].reshape(512, 128)
                    for t in some
                ],
                axis=1,
            )
            term = mm(lhs, x)
            for k in range(len(some)):
                unit.put(at + k, term[:, k * 128 : (k + 1) * 128])
        unit.step_core()

    def back_part(q, planes):
        near, far = None, None
        for a in planes:
            for b in range(3):
                x = cd[q + 2 - a, 2 - b : 10 - b].reshape(256, 256)
                one = mm(x, ckt[3 * a + b, :, 0:256])
                two = mm(x, ckt[3 * a + b, :, 256:384])
                near = one if near is None else near + one
                far = two if far is None else far + two
        return near, far

    cacc[0], spr[0, 0:256] = back_part(0, (0, 1))
    for unit in coarse_units[: len(coarse_units) // 2]:
        unit.step_a()
    cacc[1], spr[1, 0:256] = back_part(1, (1, 2))
    for unit in coarse_units[len(coarse_units) // 2 :]:
        unit.step_a()

    def fine_planes(q):
        neighbour(cd, sem_c, q).wait_recv()

        @pl.when(i == 63 * q)
        def _():
            cd[3 * q, 1:9] = jnp.zeros((8, 32, 256), BF16)

        near, far = back_part(q, (2,) if q == 0 else (0,))
        near, far = near + cacc[q], far + spr[q, 0:256]
        grad = near[:, 128:] + shift_rows(near[:, :128], -1, 32) + shift_rows(far, 1, 32)
        grad = grad.astype(BF16).astype(F32) * 0.125
        spr[q, pl.ds(0, 256, stride=2), :] = grad
        spr[q, pl.ds(1, 256, stride=2), :] = grad
        wide = spr[q]
        for p in (2 * q, 2 * q + 1):
            d = (beside(wide, wide) * slope[p]).astype(BF16)
            for k in range(2):
                dt[k, :, p * 512 : (p + 1) * 512] = mm_nt(picks[2 + k], d).astype(BF16)

    fine_planes(0)
    fine_planes(1)

    def before(a, c):
        return v[c, a : a + 4, 0:8, :, 128:256].reshape(2048, 128)

    def after(a, c):
        return v[c, a : a + 4, 2:10, :, 0:128].reshape(2048, 128)

    def fine_groups(unit, groups, at, count):
        k = 0 if unit.first == "z" else 1
        some = groups[at : at + count]
        if count == 2:
            low = mm(dt[k, 0:128], beside(*(before(*g) for g in some)))
            high = mm(dt[k, 128:256], beside(*(after(*g) for g in some)))
            lows = low[:, :128], low[:, 128:]
            highs = high[:, :128], high[:, 128:]
        else:
            both = mm(dt[k], beside(before(*some[0]), after(*some[0])))
            lows, highs = (both[:128, :128],), (both[128:, 128:],)
        for j, (a, c) in enumerate(some):
            mid = mm(dt[k], v[c, a : a + 4, 1:9].reshape(2048, 256))
            tap = 3 * (at + j)
            unit.put(tap, mid[128:, :128] + lows[j])
            unit.put(tap + 1, mid[:128, :128] + mid[128:, 128:])
            unit.put(tap + 2, mid[:128, 128:] + highs[j])
    one, two, three = fine_units
    groups = [unit[-1] for unit in FINE_UNITS]
    fine_groups(one, groups[0], 0, 2)
    fine_groups(one, groups[0], 2, 2)
    one.step_core()
    for unit in coarse_units:
        unit.step_ring()
    fine_groups(two, groups[1], 0, 2)
    one.step_a()
    fine_groups(two, groups[1], 2, 1)
    two.step_core()
    fine_groups(three, groups[2], 0, 2)
    three.step_core()
    two.step_a()
    for unit in coarse_units:
        unit.step_b()
    three.step_a()
    one.step_b()
    two.step_b()
    three.step_b()
    for unit in coarse_units:
        unit.step_c(coarse_out)
    one.step_c(fine_out)
    two.step_c(fine_out)
    for unit in coarse_units:
        unit.step_d(coarse_out)
    one.step_d(fine_out)
    three.step_c(fine_out)
    for side in range(2):
        for e in range(2):
            halo(side, e).wait_send()
        neighbour(pc.at[1], sem_p, side).wait_send()
        neighbour(cd, sem_c, side).wait_send()
    store_out.wait()


def finish(*refs):
    ins, outs, bufs, sem = refs[:3], refs[3:6], refs[6:9], refs[9]
    reads = [pltpu.make_async_copy(ins[k], bufs[k], sem.at[0, k]) for k in range(3)]
    writes = [pltpu.make_async_copy(bufs[k], outs[k], sem.at[1, k]) for k in range(3)]
    for read in reads:
        read.start()
    for read, write in zip(reads, writes):
        read.wait()
        write.start()
    for write in writes:
        write.wait()


def shards(volumes, fine_kernel, coarse_kernel, cotangent):
    vol = volumes.reshape(4, 8, 2, 64, 128)
    any_spec = pl.BlockSpec(memory_space=pl.ANY)
    vmem = pl.BlockSpec(memory_space=pltpu.VMEM)
    scratch = [
        pltpu.VMEM((3, 6, 10, 64, 256), BF16),
        pltpu.VMEM((27, 128, 128), BF16),
        pltpu.VMEM((27, 128, 256), BF16),
        pltpu.VMEM((2, 8, 32, 256), BF16),
        pltpu.VMEM((4, 512, 256), F32),
        pltpu.VMEM((2, 512, 128), F32),
        pltpu.VMEM((2, 512, 128), F32),
        pltpu.VMEM((3, 4, 10, 32, 128), BF16),
        pltpu.VMEM((4, 10, 32, 256), BF16),
        pltpu.VMEM((2, 256, 256), F32),
        pltpu.VMEM((2, 8, 32, 256), BF16),
        pltpu.VMEM((2, 256, 2048), BF16),
        pltpu.VMEM((2, 512, 256), F32),
        pltpu.VMEM((9, 256, 384), BF16),
        pltpu.VMEM((4, 256, 256), BF16),
        pltpu.SemaphoreType.DMA((5,)),
        pltpu.SemaphoreType.DMA,
        pltpu.SemaphoreType.DMA((2, 2, 2)),
        pltpu.SemaphoreType.DMA((2, 2)),
        pltpu.SemaphoreType.DMA((2, 2)),
    ]
    for *_, taps in COARSE_UNITS:
        scratch += unit_scratch(taps, 4)
    for *_, groups in FINE_UNITS:
        scratch += unit_scratch(fine_taps(groups), 2)
    results = (
        jax.ShapeDtypeStruct((2, 8, 32, 256), BF16),
        jax.ShapeDtypeStruct((2, 3456), F32),
        jax.ShapeDtypeStruct((4, 3456), F32),
    )
    made = pl.pallas_call(
        kernel,
        out_shape=results,
        in_specs=[any_spec] * 4,
        out_specs=(any_spec, vmem, vmem),
        scratch_shapes=scratch,
        compiler_params=pltpu.CompilerParams(
            collective_id=0, has_side_effects=True, vmem_limit_bytes=60 * 2**20
        ),
        name="unet_step",
    )(vol, fine_kernel, coarse_kernel, cotangent[0])
    out, fine, coarse = pl.pallas_call(
        finish,
        out_shape=results,
        in_specs=[any_spec] * 3,
        out_specs=[any_spec] * 3,
        scratch_shapes=[pltpu.VMEM(r.shape, r.dtype) for r in results]
        + [pltpu.SemaphoreType.DMA((2, 3))],
        name="finish",
    )(*made)
    return out[None], fine, coarse


def solution(mesh):
    in_specs = (
        P("sample", "space", None, None, None),
        P(),
        P(),
        P("sample", "space", None, None, None),
    )
    out_specs = (P("sample", "space", None, None, None), P("space", None), P("space", None))
    return jax.shard_map(
        shards, mesh=mesh, in_specs=in_specs, out_specs=out_specs, check_vma=False
    )
```

```python
import jax
import jax.numpy as jnp
from jax import lax
from jax.experimental import pallas as pl
from jax.experimental.pallas import tpu as pltpu
from jax.sharding import PartitionSpec as P

F32 = jnp.float32
BF16 = jnp.bfloat16
MESH = pl.DeviceIdType.MESH
NT = (((1,), (1,)), ((), ()))

COARSE_UNITS = (
    ("z", True, False, tuple(range(14))),
    ("y", True, False, tuple(range(14, 27))),
)
FINE_UNITS = (
    ("z", False, False, ((0, 0), (0, 1), (0, 2), (1, 0))),
    ("y", False, True, ((1, 1), (1, 2), (2, 0))),
    ("z", False, True, ((2, 1), (2, 2))),
)


def fine_taps(groups):
    return tuple(9 * a + 3 * b + c for a, c in groups for b in range(3))


def mm(x, w):
    return jnp.dot(x, w, preferred_element_type=F32)


def mm_nt(x, w):
    return lax.dot_general(x, w, NT, preferred_element_type=F32)


def sigmoid(v):
    return 1.0 / (1.0 + jnp.exp(-v))


def up16(n):
    return -(-n // 16) * 16


def place():
    s = lax.axis_index("sample")
    i = lax.axis_index("space")
    return s, i // 32, (i // 8) % 4, (i // 2) % 4, i % 2


def device(s, xl, y, z, core):
    return (s, ((xl * 4 + y) * 4 + z) * 2 + core)


def moved(ds, dxl, dy, dz, dcore):
    s, xl, y, z, core = place()
    return device(
        (s + ds) % 2, (xl + dxl) % 2, (y + dy) % 4, (z + dz) % 4, (core + dcore) % 2
    )


def b_moves():
    return [
        (do, dxl, ds) for do in range(4) for dxl in range(2) for ds in range(2)
    ]


def permutation(rows, first, width):
    s, xl, y, z, core = place()
    m = lax.broadcasted_iota(jnp.int32, (rows, width), 0)
    o = lax.broadcasted_iota(jnp.int32, (rows, width), 1)
    r = width // 64
    group = m // r
    mxl = (group % 2 + xl) % 2
    other = (group // 2) % 4
    lead = (group // 8) % 4
    mcore = ((group // 32) % 2 + core) % 2
    if first == "z":
        mz, my = (lead + z) % 4, (other + y) % 4
    else:
        mz, my = (other + z) % 4, (lead + y) % 4
    shard = ((mxl * 4 + my) * 4 + mz) * 2 + mcore
    return (shard * r + m % r == o).astype(F32).astype(BF16)


class Unit:
    def __init__(self, first, ring, twice, taps, rows, refs):
        self.first, self.ring, self.twice, self.taps, self.rows = first, ring, twice, taps, rows
        (self.own, self.send0, self.recv0, self.senda, self.recva, self.sendb, self.recvb,
         self.sendc, self.sem0, self.sema, self.semb, self.semc) = refs
        self.half = 32 * rows
        self.chunk = 8 * rows
        self.fold = up16(len(taps) * rows)
        width = len(taps) * 128
        low = len(taps) // 2 * 128
        self.low, self.high = pl.ds(0, low), pl.ds(low, width - low)

    def put(self, j, value):
        lanes = pl.ds(j * 128, 128)
        self.own[:, lanes] = value[: self.half]
        self.send0[:, lanes] = value[self.half :].astype(BF16)

    def core_copy(self):
        return pltpu.make_async_remote_copy(
            self.send0, self.recv0, self.sem0.at[0], self.sem0.at[1],
            device_id=moved(0, 0, 0, 0, 1), device_id_type=MESH,
        )

    def lead(self, d):
        return moved(0, 0, 0, d, 0) if self.first == "z" else moved(0, 0, d, 0, 0)

    def a_copy(self, d):
        return pltpu.make_async_remote_copy(
            self.senda.at[d - 1], self.recva.at[d - 1],
            self.sema.at[0, d - 1], self.sema.at[1, d - 1],
            device_id=self.lead(d), device_id_type=MESH,
        )

    def r_copy(self, k):
        slot, lanes, d = (
            (1, self.low, 1), (1, self.high, 3), (0, self.high, 1), (2, self.low, 3),
            (0, self.low, 1), (2, self.high, 3),
        )[k]
        return pltpu.make_async_remote_copy(
            self.senda.at[slot, :, lanes], self.recva.at[slot, :, lanes],
            self.sema.at[0, k], self.sema.at[1, k],
            device_id=self.lead(d), device_id_type=MESH,
        )

    def b_copy(self, move):
        do, dxl, ds = move
        slot = (do * 4 + dxl * 2 + ds if self.twice else do * 2 + dxl) - 1
        to = moved(ds, dxl, do, 0, 0) if self.first == "z" else moved(ds, dxl, 0, do, 0)
        return pltpu.make_async_remote_copy(
            self.sendb.at[do * 2 + dxl], self.recvb.at[slot],
            self.semb.at[0, slot], self.semb.at[1, slot],
            device_id=to, device_id_type=MESH,
        )

    def c_copy(self):
        return pltpu.make_async_remote_copy(
            self.sendc.at[0], self.sendc.at[1], self.semc.at[0], self.semc.at[1],
            device_id=moved(1, 0, 0, 0, 0), device_id_type=MESH,
        )

    def b_moves(self):
        return [m for m in b_moves()[1:] if self.twice or m[2] == 0]

    def rows_of(self, d):
        return pl.ds(d * self.chunk, self.chunk)

    def step_core(self):
        self.core_copy().start()

    def step_a(self):
        self.core_copy().wait()
        if not self.ring:
            for d in (2, 1, 3):
                self.senda[d - 1] = self.summed(d).astype(BF16)
                self.a_copy(d).start()
            self.own[self.rows_of(0), :] = self.summed(0)
            return
        self.senda[1] = self.summed(2).astype(BF16)
        for k in range(2):
            self.r_copy(k).start()
        for d in (1, 3, 0):
            self.own[self.rows_of(d), :] = self.summed(d)
        self.senda[0, :, self.high] = self.own[self.rows_of(1), self.high].astype(BF16)
        self.senda[2, :, self.low] = self.own[self.rows_of(3), self.low].astype(BF16)
        for k in range(2, 4):
            self.r_copy(k).start()

    def summed(self, d):
        rows = self.rows_of(d)
        return self.own[rows, :] + self.recv0[rows, :].astype(F32)

    def step_ring(self):
        for k in range(2):
            self.r_copy(k).wait()
        one = self.own[self.rows_of(1), self.low] + self.recva[1, :, self.low].astype(F32)
        self.senda[0, :, self.low] = one.astype(BF16)
        three = self.own[self.rows_of(3), self.high] + self.recva[1, :, self.high].astype(F32)
        self.senda[2, :, self.high] = three.astype(BF16)
        for k in range(4, 6):
            self.r_copy(k).start()

    def step_b(self):
        total = self.own[self.rows_of(0), :]
        if self.ring:
            for k in range(2, 6):
                self.r_copy(k).wait()
            total = total + self.recva[0].astype(F32) + self.recva[2].astype(F32)
        else:
            for d in range(1, 4):
                self.a_copy(d).wait()
            for d in range(1, 4):
                total = total + self.recva[d - 1].astype(F32)
        r = self.rows
        for q in (4, 5, 2, 3, 6, 7, 1, 0):
            rows = total[q * r : (q + 1) * r]
            pieces = [rows[:, j * 128 : (j + 1) * 128] for j in range(len(self.taps))]
            missing = self.fold - r * len(self.taps)
            if missing:
                pieces.append(jnp.zeros((missing, 128), F32))
            self.sendb[q] = jnp.concatenate(pieces, axis=0).astype(BF16)
            for move in self.b_moves():
                if move[0] * 2 + move[1] == q:
                    self.b_copy(move).start()

    def emit(self, total, out):
        r = self.rows
        for j, tap in enumerate(self.taps):
            out[:, tap * 128 : (tap + 1) * 128] = total[j * r : (j + 1) * r]

    def step_c(self, out):
        for move in self.b_moves():
            self.b_copy(move).wait()
        total = self.sendb[0].astype(F32)
        if self.twice:
            total = total + self.recvb[0].astype(F32)
            for k in range(1, 14, 2):
                total = total + (self.recvb[k].astype(F32) + self.recvb[k + 1].astype(F32))
            self.emit(total, out)
        else:
            for k in range(7):
                total = total + self.recvb[k].astype(F32)
            self.sendc[0] = total.astype(BF16)
            self.c_copy().start()

    def step_d(self, out):
        self.c_copy().wait()
        self.emit(self.sendc[0].astype(F32) + self.sendc[1].astype(F32), out)


def unit_scratch(taps, rows):
    width, half, chunk = len(taps) * 128, 32 * rows, 8 * rows
    fold = up16(len(taps) * rows)
    return [
        pltpu.VMEM((half, width), F32),
        pltpu.VMEM((half, width), BF16),
        pltpu.VMEM((half, width), BF16),
        pltpu.VMEM((3, chunk, width), BF16),
        pltpu.VMEM((3, chunk, width), BF16),
        pltpu.VMEM((8, fold, 128), BF16),
        pltpu.VMEM((15, fold, 128), BF16),
        pltpu.VMEM((2, fold, 128), BF16),
        pltpu.SemaphoreType.DMA((2,)),
        pltpu.SemaphoreType.DMA((2, 6)),
        pltpu.SemaphoreType.DMA((2, 15)),
        pltpu.SemaphoreType.DMA((2,)),
    ]


def shift_rows(block, step, period):
    size = block.shape[0]
    row = lax.broadcasted_iota(jnp.int32, block.shape, 0) % period
    if step > 0:
        return jnp.where(row == 0, 0.0, pltpu.roll(block, 1, 0))
    return jnp.where(row == period - 1, 0.0, pltpu.roll(block, size - 1, 0))


def kernel(
    vol, fk_hbm, ck_hbm, ct_hbm,
    out_hbm, fine_out, coarse_out,
    v, fk, ck, ct, slope, pool, spr, pc, cd, cacc, outb, dt, facc, ckt, picks,
    sem_in, sem_out, sem_v, sem_p, sem_c,
    *unit_refs,
):
    s, i = lax.axis_index("sample"), lax.axis_index("space")
    left = (s, (i + 63) % 64)
    right = (s, (i + 1) % 64)
    units = []
    at = 0
    for *how, taps in COARSE_UNITS:
        units.append(Unit(*how, taps, 4, unit_refs[at : at + 12]))
        at += 12
    for *how, groups in FINE_UNITS:
        units.append(Unit(*how, fine_taps(groups), 2, unit_refs[at : at + 12]))
        at += 12
    coarse_units, fine_units = units[: len(COARSE_UNITS)], units[len(COARSE_UNITS) :]

    barrier = pltpu.get_barrier_semaphore()
    moves = {(ds, dxl, do, 0, 0) for do, dxl, ds in b_moves()}
    moves |= {(ds, dxl, 0, do, 0) for do, dxl, ds in b_moves()}
    moves.discard((0, 0, 0, 0, 0))
    moves.add((0, 0, 0, 0, 1))
    peers = [left, right] + [moved(*move) for move in sorted(moves)]
    for peer in peers[:2]:
        pl.semaphore_signal(barrier, inc=1, device_id=peer, device_id_type=MESH)

    def interior(e):
        return pltpu.make_async_copy(
            vol.at[:, :, e],
            v.at[1, pl.ds(1, 4), pl.ds(1, 8), :, pl.ds(e * 128, 128)],
            sem_in.at[e],
        )

    load_fk = pltpu.make_async_copy(fk_hbm, fk, sem_in.at[2])
    load_ck = pltpu.make_async_copy(ck_hbm, ck, sem_in.at[3])
    load_ct = pltpu.make_async_copy(ct_hbm, ct, sem_in.at[4])
    interior(0).start()
    interior(1).start()
    load_fk.start()
    load_ck.start()
    load_ct.start()
    for peer in peers[2:]:
        pl.semaphore_signal(barrier, inc=1, device_id=peer, device_id_type=MESH)

    def halo(side, e):
        return pltpu.make_async_remote_copy(
            v.at[1, 4 if side == 0 else 1, pl.ds(1, 8), :, pl.ds(e * 128, 128)],
            v.at[1, 0 if side == 0 else 5, pl.ds(1, 8), :, pl.ds(e * 128, 128)],
            sem_v.at[0, side, e], sem_v.at[1, side, e],
            device_id=right if side == 0 else left, device_id_type=MESH,
        )

    for c in range(3):
        for p in range(6):
            v[c, p, 0] = jnp.zeros((64, 256), BF16)
            v[c, p, 9] = jnp.zeros((64, 256), BF16)
        for p in range(4):
            pc[c, p, 0] = jnp.zeros((32, 128), BF16)
            pc[c, p, 9] = jnp.zeros((32, 128), BF16)
    for p in range(4):
        cd[p, 0] = jnp.zeros((32, 256), BF16)
        cd[p, 9] = jnp.zeros((32, 256), BF16)

    def shift_fine(p):
        block = v[1, p, 1:9].reshape(512, 256).astype(F32)
        v[0, p, 1:9] = shift_rows(block, 1, 64).astype(BF16).reshape(8, 64, 256)
        v[2, p, 1:9] = shift_rows(block, -1, 64).astype(BF16).reshape(8, 64, 256)

    for k, first in enumerate(("z", "y")):
        picks[k] = permutation(256, first, 256)
        pick = permutation(128, first, 128)
        none = jnp.zeros((128, 128), BF16)
        picks[2 + k, 0:128, 0:128] = pick
        picks[2 + k, 0:128, 128:256] = none
        picks[2 + k, 128:256, 0:128] = none
        picks[2 + k, 128:256, 128:256] = pick
    interior(0).wait()
    interior(1).wait()
    pl.semaphore_wait(barrier, len(peers))
    for side in range(2):
        for e in range(2):
            halo(side, e).start()
    for p in range(1, 5):
        shift_fine(p)
    load_fk.wait()

    zero = jnp.zeros((128, 128), BF16)

    def beside(a, b):
        return jnp.concatenate([a, b], axis=1)

    def over(a, b):
        return jnp.concatenate([a, b], axis=0)

    def fine_part(p, planes):
        acc = None
        for a in planes:
            for c in range(3):
                k0, k1, k2 = (fk[9 * a + 3 * b + c] for b in range(3))
                here = v[c, p + a, 1:9].reshape(512, 256)
                around = beside(
                    v[c, p + a, 0:8, :, 128:256].reshape(512, 128),
                    v[c, p + a, 2:10, :, 0:128].reshape(512, 128),
                )
                term = mm(here, over(beside(k1, k0), beside(k2, k1)))
                term = term + mm(around, over(beside(k0, zero), beside(zero, k2)))
                acc = term if acc is None else acc + term
        return acc

    def fine_forward(p, acc):
        sig = sigmoid(acc)
        act = acc * sig
        slope[p] = sig + act * (1.0 - sig)
        return act[:, :128] + act[:, 128:]

    def shift_pooled(p):
        block = pc[1, p, 1:9].reshape(256, 128).astype(F32)
        pc[0, p, 1:9] = shift_rows(block, 1, 32).astype(BF16).reshape(8, 32, 128)
        pc[2, p, 1:9] = shift_rows(block, -1, 32).astype(BF16).reshape(8, 32, 128)

    def pool_plane(q):
        even = pool[q, pl.ds(0, 256, stride=2), :]
        odd = pool[q, pl.ds(1, 256, stride=2), :]
        pc[1, q + 1, 1:9] = ((even + odd) * 0.125).astype(BF16).reshape(8, 32, 128)

    def neighbour(ref, sems, side):
        return pltpu.make_async_remote_copy(
            ref.at[2 if side == 0 else 1, pl.ds(1, 8)],
            ref.at[0 if side == 0 else 3, pl.ds(1, 8)],
            sems.at[0, side], sems.at[1, side],
            device_id=right if side == 0 else left, device_id_type=MESH,
        )

    pool[0] = fine_forward(1, fine_part(1, (0, 1, 2)))
    pool[1] = fine_forward(2, fine_part(2, (0, 1, 2)))
    facc[0] = fine_part(0, (1, 2))
    facc[1] = fine_part(3, (0, 1))
    for e in range(2):
        halo(0, e).wait_recv()

    @pl.when(i == 0)
    def _():
        v[1, 0, 1:9] = jnp.zeros((8, 64, 256), BF16)

    shift_fine(0)
    pool[0] = pool[0] + fine_forward(0, facc[0] + fine_part(0, (0,)))
    pool_plane(0)
    neighbour(pc.at[1], sem_p, 1).start()
    for e in range(2):
        halo(1, e).wait_recv()

    @pl.when(i == 63)
    def _():
        v[1, 5, 1:9] = jnp.zeros((8, 64, 256), BF16)

    shift_fine(5)
    pool[1] = pool[1] + fine_forward(3, facc[1] + fine_part(3, (2,)))
    pool_plane(1)
    neighbour(pc.at[1], sem_p, 0).start()
    shift_pooled(1)
    shift_pooled(2)
    load_ck.wait()
    load_ct.wait()

    def piece(q, a, b, c):
        return pc[c, q + a, b : b + 8].reshape(256, 128)

    def coarse_part(q, planes):
        taps = [(a, b, c) for a in planes for b in range(3) for c in range(3)]
        acc = None
        for at in range(0, len(taps), 2):
            some = taps[at : at + 2]
            x = jnp.concatenate([piece(q, *tap) for tap in some], axis=1)
            w = jnp.concatenate([ck[9 * a + 3 * b + c] for a, b, c in some], axis=0)
            term = mm(x, w)
            acc = term if acc is None else acc + term
        return acc

    cacc[0] = coarse_part(0, (1, 2))
    cacc[1] = coarse_part(1, (0, 1))
    for t in range(27):
        ckt[t // 3, :, t % 3 * 128 : t % 3 * 128 + 128] = ck[t].T
    def coarse_plane(q):
        neighbour(pc.at[1], sem_p, q).wait_recv()

        @pl.when(i == 63 * q)
        def _():
            pc[1, 3 * q, 1:9] = jnp.zeros((8, 32, 128), BF16)

        shift_pooled(3 * q)
        pre = cacc[q] + coarse_part(q, (0,) if q == 0 else (2,))
        sig = sigmoid(pre)
        act = pre * sig
        outb[q] = act.astype(BF16).reshape(8, 32, 256)
        grad = ct[q].reshape(256, 256).astype(F32)
        cd[q + 1, 1:9] = (grad * (sig + act * (1.0 - sig))).astype(BF16).reshape(8, 32, 256)
        neighbour(cd, sem_c, 1 - q).start()

    coarse_plane(0)
    coarse_plane(1)
    store_out = pltpu.make_async_copy(outb, out_hbm, sem_out)
    store_out.start()

    delta = cd[1:3, 1:9].reshape(512, 256)
    orders = {
        first: mm_nt(picks[k], delta).astype(BF16) for k, first in enumerate(("z", "y"))
    }
    for unit in coarse_units:
        lhs = orders[unit.first]
        for at in range(0, len(unit.taps), 2):
            some = unit.taps[at : at + 2]
            x = jnp.concatenate(
                [
                    pc[t % 3, t // 9 : t // 9 + 2, t // 3 % 3 : t // 3 % 3 + 8].reshape(512, 128)
                    for t in some
                ],
                axis=1,
            )
            term = mm(lhs, x)
            for k in range(len(some)):
                unit.put(at + k, term[:, k * 128 : (k + 1) * 128])
        unit.step_core()

    def back_part(q, planes):
        near, far = None, None
        for a in planes:
            for b in range(3):
                x = cd[q + 2 - a, 2 - b : 10 - b].reshape(256, 256)
                one = mm(x, ckt[3 * a + b, :, 0:256])
                two = mm(x, ckt[3 * a + b, :, 256:384])
                near = one if near is None else near + one
                far = two if far is None else far + two
        return near, far

    cacc[0], spr[0, 0:256] = back_part(0, (0, 1))
    for unit in coarse_units[: len(coarse_units) // 2]:
        unit.step_a()
    cacc[1], spr[1, 0:256] = back_part(1, (1, 2))
    for unit in coarse_units[len(coarse_units) // 2 :]:
        unit.step_a()

    def fine_planes(q):
        neighbour(cd, sem_c, q).wait_recv()

        @pl.when(i == 63 * q)
        def _():
            cd[3 * q, 1:9] = jnp.zeros((8, 32, 256), BF16)

        near, far = back_part(q, (2,) if q == 0 else (0,))
        near, far = near + cacc[q], far + spr[q, 0:256]
        grad = near[:, 128:] + shift_rows(near[:, :128], -1, 32) + shift_rows(far, 1, 32)
        grad = grad.astype(BF16).astype(F32) * 0.125
        spr[q, pl.ds(0, 256, stride=2), :] = grad
        spr[q, pl.ds(1, 256, stride=2), :] = grad
        wide = spr[q]
        for p in (2 * q, 2 * q + 1):
            d = (beside(wide, wide) * slope[p]).astype(BF16)
            for k in range(2):
                dt[k, :, p * 512 : (p + 1) * 512] = mm_nt(picks[2 + k], d).astype(BF16)

    fine_planes(0)
    fine_planes(1)

    def before(a, c):
        return v[c, a : a + 4, 0:8, :, 128:256].reshape(2048, 128)

    def after(a, c):
        return v[c, a : a + 4, 2:10, :, 0:128].reshape(2048, 128)

    def fine_groups(unit, groups, at, count):
        k = 0 if unit.first == "z" else 1
        some = groups[at : at + count]
        if count == 2:
            low = mm(dt[k, 0:128], beside(*(before(*g) for g in some)))
            high = mm(dt[k, 128:256], beside(*(after(*g) for g in some)))
            lows = low[:, :128], low[:, 128:]
            highs = high[:, :128], high[:, 128:]
        else:
            both = mm(dt[k], beside(before(*some[0]), after(*some[0])))
            lows, highs = (both[:128, :128],), (both[128:, 128:],)
        for j, (a, c) in enumerate(some):
            mid = mm(dt[k], v[c, a : a + 4, 1:9].reshape(2048, 256))
            tap = 3 * (at + j)
            unit.put(tap, mid[128:, :128] + lows[j])
            unit.put(tap + 1, mid[:128, :128] + mid[128:, 128:])
            unit.put(tap + 2, mid[:128, 128:] + highs[j])
    one, two, three = fine_units
    groups = [unit[-1] for unit in FINE_UNITS]
    fine_groups(one, groups[0], 0, 2)
    coarse_units[0].step_ring()
    fine_groups(one, groups[0], 2, 2)
    one.step_core()
    coarse_units[1].step_ring()
    fine_groups(two, groups[1], 0, 2)
    one.step_a()
    fine_groups(two, groups[1], 2, 1)
    two.step_core()
    fine_groups(three, groups[2], 0, 2)
    three.step_core()
    two.step_a()
    for unit in coarse_units:
        unit.step_b()
    three.step_a()
    one.step_b()
    two.step_b()
    three.step_b()
    for unit in coarse_units:
        unit.step_c(coarse_out)
    one.step_c(fine_out)
    two.step_c(fine_out)
    for unit in coarse_units:
        unit.step_d(coarse_out)
    one.step_d(fine_out)
    three.step_c(fine_out)
    for side in range(2):
        for e in range(2):
            halo(side, e).wait_send()
        neighbour(pc.at[1], sem_p, side).wait_send()
        neighbour(cd, sem_c, side).wait_send()
    store_out.wait()


def finish(*refs):
    ins, outs, bufs, sem = refs[:3], refs[3:6], refs[6:9], refs[9]
    reads = [pltpu.make_async_copy(ins[k], bufs[k], sem.at[0, k]) for k in range(3)]
    writes = [pltpu.make_async_copy(bufs[k], outs[k], sem.at[1, k]) for k in range(3)]
    for read in reads:
        read.start()
    for read, write in zip(reads, writes):
        read.wait()
        write.start()
    for write in writes:
        write.wait()


def shards(volumes, fine_kernel, coarse_kernel, cotangent):
    vol = volumes.reshape(4, 8, 2, 64, 128)
    any_spec = pl.BlockSpec(memory_space=pl.ANY)
    vmem = pl.BlockSpec(memory_space=pltpu.VMEM)
    scratch = [
        pltpu.VMEM((3, 6, 10, 64, 256), BF16),
        pltpu.VMEM((27, 128, 128), BF16),
        pltpu.VMEM((27, 128, 256), BF16),
        pltpu.VMEM((2, 8, 32, 256), BF16),
        pltpu.VMEM((4, 512, 256), F32),
        pltpu.VMEM((2, 512, 128), F32),
        pltpu.VMEM((2, 512, 128), F32),
        pltpu.VMEM((3, 4, 10, 32, 128), BF16),
        pltpu.VMEM((4, 10, 32, 256), BF16),
        pltpu.VMEM((2, 256, 256), F32),
        pltpu.VMEM((2, 8, 32, 256), BF16),
        pltpu.VMEM((2, 256, 2048), BF16),
        pltpu.VMEM((2, 512, 256), F32),
        pltpu.VMEM((9, 256, 384), BF16),
        pltpu.VMEM((4, 256, 256), BF16),
        pltpu.SemaphoreType.DMA((5,)),
        pltpu.SemaphoreType.DMA,
        pltpu.SemaphoreType.DMA((2, 2, 2)),
        pltpu.SemaphoreType.DMA((2, 2)),
        pltpu.SemaphoreType.DMA((2, 2)),
    ]
    for *_, taps in COARSE_UNITS:
        scratch += unit_scratch(taps, 4)
    for *_, groups in FINE_UNITS:
        scratch += unit_scratch(fine_taps(groups), 2)
    results = (
        jax.ShapeDtypeStruct((2, 8, 32, 256), BF16),
        jax.ShapeDtypeStruct((2, 3456), F32),
        jax.ShapeDtypeStruct((4, 3456), F32),
    )
    made = pl.pallas_call(
        kernel,
        out_shape=results,
        in_specs=[any_spec] * 4,
        out_specs=(any_spec, vmem, vmem),
        scratch_shapes=scratch,
        compiler_params=pltpu.CompilerParams(
            collective_id=0, has_side_effects=True, vmem_limit_bytes=60 * 2**20
        ),
        name="unet_step",
    )(vol, fine_kernel, coarse_kernel, cotangent[0])
    out, fine, coarse = pl.pallas_call(
        finish,
        out_shape=results,
        in_specs=[any_spec] * 3,
        out_specs=[any_spec] * 3,
        scratch_shapes=[pltpu.VMEM(r.shape, r.dtype) for r in results]
        + [pltpu.SemaphoreType.DMA((2, 3))],
        name="finish",
    )(*made)
    return out[None], fine, coarse


def solution(mesh):
    in_specs = (
        P("sample", "space", None, None, None),
        P(),
        P(),
        P("sample", "space", None, None, None),
    )
    out_specs = (P("sample", "space", None, None, None), P("space", None), P("space", None))
    return jax.shard_map(
        shards, mesh=mesh, in_specs=in_specs, out_specs=out_specs, check_vma=False
    )
```

```python
import jax
import jax.numpy as jnp
from jax import lax
from jax.experimental import pallas as pl
from jax.experimental.pallas import tpu as pltpu
from jax.sharding import PartitionSpec as P

F32 = jnp.float32
BF16 = jnp.bfloat16
MESH = pl.DeviceIdType.MESH
NT = (((1,), (1,)), ((), ()))

COARSE_UNITS = (
    ("z", True, False, tuple(range(14))),
    ("y", True, False, tuple(range(14, 27))),
)
FINE_UNITS = (
    ("z", False, False, ((0, 0), (0, 1), (0, 2), (1, 0))),
    ("y", False, True, ((1, 1), (1, 2), (2, 0))),
    ("z", False, True, ((2, 1), (2, 2))),
)


def fine_taps(groups):
    return tuple(9 * a + 3 * b + c for a, c in groups for b in range(3))


def mm(x, w):
    return jnp.dot(x, w, preferred_element_type=F32)


def mm_nt(x, w):
    return lax.dot_general(x, w, NT, preferred_element_type=F32)


def sigmoid(v):
    return 1.0 / (1.0 + jnp.exp(-v))


def up16(n):
    return -(-n // 16) * 16


def place():
    s = lax.axis_index("sample")
    i = lax.axis_index("space")
    return s, i // 32, (i // 8) % 4, (i // 2) % 4, i % 2


def device(s, xl, y, z, core):
    return (s, ((xl * 4 + y) * 4 + z) * 2 + core)


def moved(ds, dxl, dy, dz, dcore):
    s, xl, y, z, core = place()
    return device(
        (s + ds) % 2, (xl + dxl) % 2, (y + dy) % 4, (z + dz) % 4, (core + dcore) % 2
    )


def b_moves():
    return [
        (do, dxl, ds) for do in range(4) for dxl in range(2) for ds in range(2)
    ]


def permutation(rows, first, width):
    s, xl, y, z, core = place()
    m = lax.broadcasted_iota(jnp.int32, (rows, width), 0)
    o = lax.broadcasted_iota(jnp.int32, (rows, width), 1)
    r = width // 64
    group = m // r
    mxl = (group % 2 + xl) % 2
    other = (group // 2) % 4
    lead = (group // 8) % 4
    mcore = ((group // 32) % 2 + core) % 2
    if first == "z":
        mz, my = (lead + z) % 4, (other + y) % 4
    else:
        mz, my = (other + z) % 4, (lead + y) % 4
    shard = ((mxl * 4 + my) * 4 + mz) * 2 + mcore
    return (shard * r + m % r == o).astype(F32).astype(BF16)


class Unit:
    def __init__(self, first, ring, twice, taps, rows, refs):
        self.first, self.ring, self.twice, self.taps, self.rows = first, ring, twice, taps, rows
        (self.own, self.send0, self.recv0, self.senda, self.recva, self.sendb, self.recvb,
         self.sendc, self.sem0, self.sema, self.semb, self.semc) = refs
        self.half = 32 * rows
        self.chunk = 8 * rows
        self.fold = up16(len(taps) * rows)
        width = len(taps) * 128
        low = len(taps) // 2 * 128
        self.low, self.high = pl.ds(0, low), pl.ds(low, width - low)

    def put(self, j, value):
        lanes = pl.ds(j * 128, 128)
        self.own[:, lanes] = value[: self.half]
        self.send0[:, lanes] = value[self.half :].astype(BF16)

    def core_copy(self):
        return pltpu.make_async_remote_copy(
            self.send0, self.recv0, self.sem0.at[0], self.sem0.at[1],
            device_id=moved(0, 0, 0, 0, 1), device_id_type=MESH,
        )

    def lead(self, d):
        return moved(0, 0, 0, d, 0) if self.first == "z" else moved(0, 0, d, 0, 0)

    def a_copy(self, d):
        return pltpu.make_async_remote_copy(
            self.senda.at[d - 1], self.recva.at[d - 1],
            self.sema.at[0, d - 1], self.sema.at[1, d - 1],
            device_id=self.lead(d), device_id_type=MESH,
        )

    def r_copy(self, k):
        slot, lanes, d = (
            (1, self.low, 1), (1, self.high, 3), (0, self.high, 1), (2, self.low, 3),
            (0, self.low, 1), (2, self.high, 3),
        )[k]
        return pltpu.make_async_remote_copy(
            self.senda.at[slot, :, lanes], self.recva.at[slot, :, lanes],
            self.sema.at[0, k], self.sema.at[1, k],
            device_id=self.lead(d), device_id_type=MESH,
        )

    def b_copy(self, move):
        do, dxl, ds = move
        slot = (do * 4 + dxl * 2 + ds if self.twice else do * 2 + dxl) - 1
        to = moved(ds, dxl, do, 0, 0) if self.first == "z" else moved(ds, dxl, 0, do, 0)
        return pltpu.make_async_remote_copy(
            self.sendb.at[do * 2 + dxl], self.recvb.at[slot],
            self.semb.at[0, slot], self.semb.at[1, slot],
            device_id=to, device_id_type=MESH,
        )

    def c_copy(self):
        return pltpu.make_async_remote_copy(
            self.sendc.at[0], self.sendc.at[1], self.semc.at[0], self.semc.at[1],
            device_id=moved(1, 0, 0, 0, 0), device_id_type=MESH,
        )

    def b_moves(self):
        return [m for m in b_moves()[1:] if self.twice or m[2] == 0]

    def rows_of(self, d):
        return pl.ds(d * self.chunk, self.chunk)

    def step_core(self):
        self.core_copy().start()

    def step_a(self):
        self.core_copy().wait()
        if not self.ring:
            for d in (2, 1, 3):
                self.senda[d - 1] = self.summed(d).astype(BF16)
                self.a_copy(d).start()
            self.own[self.rows_of(0), :] = self.summed(0)
            return
        self.senda[1] = self.summed(2).astype(BF16)
        for k in range(2):
            self.r_copy(k).start()
        for d in (1, 3, 0):
            self.own[self.rows_of(d), :] = self.summed(d)
        self.senda[0, :, self.high] = self.own[self.rows_of(1), self.high].astype(BF16)
        self.senda[2, :, self.low] = self.own[self.rows_of(3), self.low].astype(BF16)
        for k in range(2, 4):
            self.r_copy(k).start()

    def summed(self, d):
        rows = self.rows_of(d)
        return self.own[rows, :] + self.recv0[rows, :].astype(F32)

    def step_ring(self):
        for k in range(2):
            self.r_copy(k).wait()
        one = self.own[self.rows_of(1), self.low] + self.recva[1, :, self.low].astype(F32)
        self.senda[0, :, self.low] = one.astype(BF16)
        three = self.own[self.rows_of(3), self.high] + self.recva[1, :, self.high].astype(F32)
        self.senda[2, :, self.high] = three.astype(BF16)
        for k in range(4, 6):
            self.r_copy(k).start()

    def step_b(self):
        total = self.own[self.rows_of(0), :]
        if self.ring:
            for k in range(2, 6):
                self.r_copy(k).wait()
            total = total + self.recva[0].astype(F32) + self.recva[2].astype(F32)
        else:
            for d in range(1, 4):
                self.a_copy(d).wait()
            for d in range(1, 4):
                total = total + self.recva[d - 1].astype(F32)
        r = self.rows
        for q in (4, 5, 2, 3, 6, 7, 1, 0):
            rows = total[q * r : (q + 1) * r]
            pieces = [rows[:, j * 128 : (j + 1) * 128] for j in range(len(self.taps))]
            missing = self.fold - r * len(self.taps)
            if missing:
                pieces.append(jnp.zeros((missing, 128), F32))
            self.sendb[q] = jnp.concatenate(pieces, axis=0).astype(BF16)
            for move in self.b_moves():
                if move[0] * 2 + move[1] == q:
                    self.b_copy(move).start()

    def emit(self, total, out):
        r = self.rows
        for j, tap in enumerate(self.taps):
            out[:, tap * 128 : (tap + 1) * 128] = total[j * r : (j + 1) * r]

    def step_c(self, out):
        for move in self.b_moves():
            self.b_copy(move).wait()
        total = self.sendb[0].astype(F32)
        if self.twice:
            total = total + self.recvb[0].astype(F32)
            for k in range(1, 14, 2):
                total = total + (self.recvb[k].astype(F32) + self.recvb[k + 1].astype(F32))
            self.emit(total, out)
        else:
            for k in range(7):
                total = total + self.recvb[k].astype(F32)
            self.sendc[0] = total.astype(BF16)
            self.c_copy().start()

    def step_d(self, out):
        self.c_copy().wait()
        self.emit(self.sendc[0].astype(F32) + self.sendc[1].astype(F32), out)


def unit_scratch(taps, rows):
    width, half, chunk = len(taps) * 128, 32 * rows, 8 * rows
    fold = up16(len(taps) * rows)
    return [
        pltpu.VMEM((half, width), F32),
        pltpu.VMEM((half, width), BF16),
        pltpu.VMEM((half, width), BF16),
        pltpu.VMEM((3, chunk, width), BF16),
        pltpu.VMEM((3, chunk, width), BF16),
        pltpu.VMEM((8, fold, 128), BF16),
        pltpu.VMEM((15, fold, 128), BF16),
        pltpu.VMEM((2, fold, 128), BF16),
        pltpu.SemaphoreType.DMA((2,)),
        pltpu.SemaphoreType.DMA((2, 6)),
        pltpu.SemaphoreType.DMA((2, 15)),
        pltpu.SemaphoreType.DMA((2,)),
    ]


def shift_rows(block, step, period):
    size = block.shape[0]
    row = lax.broadcasted_iota(jnp.int32, block.shape, 0) % period
    if step > 0:
        return jnp.where(row == 0, 0.0, pltpu.roll(block, 1, 0))
    return jnp.where(row == period - 1, 0.0, pltpu.roll(block, size - 1, 0))


def kernel(
    vol, fk_hbm, ck_hbm, ct_hbm,
    out_hbm, fine_out, coarse_out,
    v, fk, ck, ct, slope, pool, spr, pc, cd, cacc, outb, dt, facc, ckt, picks,
    sem_in, sem_out, sem_v, sem_p, sem_c,
    *unit_refs,
):
    s, i = lax.axis_index("sample"), lax.axis_index("space")
    left = (s, (i + 63) % 64)
    right = (s, (i + 1) % 64)
    units = []
    at = 0
    for *how, taps in COARSE_UNITS:
        units.append(Unit(*how, taps, 4, unit_refs[at : at + 12]))
        at += 12
    for *how, groups in FINE_UNITS:
        units.append(Unit(*how, fine_taps(groups), 2, unit_refs[at : at + 12]))
        at += 12
    coarse_units, fine_units = units[: len(COARSE_UNITS)], units[len(COARSE_UNITS) :]

    barrier = pltpu.get_barrier_semaphore()
    moves = {(ds, dxl, do, 0, 0) for do, dxl, ds in b_moves()}
    moves |= {(ds, dxl, 0, do, 0) for do, dxl, ds in b_moves()}
    moves.discard((0, 0, 0, 0, 0))
    moves.add((0, 0, 0, 0, 1))
    peers = [left, right] + [moved(*move) for move in sorted(moves)]
    for peer in peers[:2]:
        pl.semaphore_signal(barrier, inc=1, device_id=peer, device_id_type=MESH)

    def interior(e):
        return pltpu.make_async_copy(
            vol.at[:, :, e],
            v.at[1, pl.ds(1, 4), pl.ds(1, 8), :, pl.ds(e * 128, 128)],
            sem_in.at[e],
        )

    load_fk = pltpu.make_async_copy(fk_hbm, fk, sem_in.at[2])
    load_ck = pltpu.make_async_copy(ck_hbm, ck, sem_in.at[3])
    load_ct = pltpu.make_async_copy(ct_hbm, ct, sem_in.at[4])
    interior(0).start()
    interior(1).start()
    load_fk.start()
    load_ck.start()
    load_ct.start()
    for peer in peers[2:]:
        pl.semaphore_signal(barrier, inc=1, device_id=peer, device_id_type=MESH)

    def halo(side, e):
        return pltpu.make_async_remote_copy(
            v.at[1, 4 if side == 0 else 1, pl.ds(1, 8), :, pl.ds(e * 128, 128)],
            v.at[1, 0 if side == 0 else 5, pl.ds(1, 8), :, pl.ds(e * 128, 128)],
            sem_v.at[0, side, e], sem_v.at[1, side, e],
            device_id=right if side == 0 else left, device_id_type=MESH,
        )

    for c in range(3):
        for p in range(6):
            v[c, p, 0] = jnp.zeros((64, 256), BF16)
            v[c, p, 9] = jnp.zeros((64, 256), BF16)
        for p in range(4):
            pc[c, p, 0] = jnp.zeros((32, 128), BF16)
            pc[c, p, 9] = jnp.zeros((32, 128), BF16)
    for p in range(4):
        cd[p, 0] = jnp.zeros((32, 256), BF16)
        cd[p, 9] = jnp.zeros((32, 256), BF16)

    def shift_fine(p):
        block = v[1, p, 1:9].reshape(512, 256).astype(F32)
        v[0, p, 1:9] = shift_rows(block, 1, 64).astype(BF16).reshape(8, 64, 256)
        v[2, p, 1:9] = shift_rows(block, -1, 64).astype(BF16).reshape(8, 64, 256)

    for k, first in enumerate(("z", "y")):
        picks[k] = permutation(256, first, 256)
        pick = permutation(128, first, 128)
        none = jnp.zeros((128, 128), BF16)
        picks[2 + k, 0:128, 0:128] = pick
        picks[2 + k, 0:128, 128:256] = none
        picks[2 + k, 128:256, 0:128] = none
        picks[2 + k, 128:256, 128:256] = pick
    interior(0).wait()
    interior(1).wait()
    pl.semaphore_wait(barrier, len(peers))
    for side in range(2):
        for e in range(2):
            halo(side, e).start()
    for p in range(1, 5):
        shift_fine(p)
    load_fk.wait()

    zero = jnp.zeros((128, 128), BF16)

    def beside(a, b):
        return jnp.concatenate([a, b], axis=1)

    def over(a, b):
        return jnp.concatenate([a, b], axis=0)

    def fine_part(p, planes):
        acc = None
        for a in planes:
            for c in range(3):
                k0, k1, k2 = (fk[9 * a + 3 * b + c] for b in range(3))
                here = v[c, p + a, 1:9].reshape(512, 256)
                around = beside(
                    v[c, p + a, 0:8, :, 128:256].reshape(512, 128),
                    v[c, p + a, 2:10, :, 0:128].reshape(512, 128),
                )
                term = mm(here, over(beside(k1, k0), beside(k2, k1)))
                term = term + mm(around, over(beside(k0, zero), beside(zero, k2)))
                acc = term if acc is None else acc + term
        return acc

    def fine_forward(p, acc):
        sig = sigmoid(acc)
        act = acc * sig
        slope[p] = sig + act * (1.0 - sig)
        return act[:, :128] + act[:, 128:]

    def shift_pooled(p):
        block = pc[1, p, 1:9].reshape(256, 128).astype(F32)
        pc[0, p, 1:9] = shift_rows(block, 1, 32).astype(BF16).reshape(8, 32, 128)
        pc[2, p, 1:9] = shift_rows(block, -1, 32).astype(BF16).reshape(8, 32, 128)

    def pool_plane(q):
        even = pool[q, pl.ds(0, 256, stride=2), :]
        odd = pool[q, pl.ds(1, 256, stride=2), :]
        pc[1, q + 1, 1:9] = ((even + odd) * 0.125).astype(BF16).reshape(8, 32, 128)

    def neighbour(ref, sems, side):
        return pltpu.make_async_remote_copy(
            ref.at[2 if side == 0 else 1, pl.ds(1, 8)],
            ref.at[0 if side == 0 else 3, pl.ds(1, 8)],
            sems.at[0, side], sems.at[1, side],
            device_id=right if side == 0 else left, device_id_type=MESH,
        )

    pool[0] = fine_forward(1, fine_part(1, (0, 1, 2)))
    pool[1] = fine_forward(2, fine_part(2, (0, 1, 2)))
    facc[0] = fine_part(0, (1, 2))
    facc[1] = fine_part(3, (0, 1))
    for e in range(2):
        halo(0, e).wait_recv()

    @pl.when(i == 0)
    def _():
        v[1, 0, 1:9] = jnp.zeros((8, 64, 256), BF16)

    shift_fine(0)
    pool[0] = pool[0] + fine_forward(0, facc[0] + fine_part(0, (0,)))
    pool_plane(0)
    neighbour(pc.at[1], sem_p, 1).start()
    for e in range(2):
        halo(1, e).wait_recv()

    @pl.when(i == 63)
    def _():
        v[1, 5, 1:9] = jnp.zeros((8, 64, 256), BF16)

    shift_fine(5)
    pool[1] = pool[1] + fine_forward(3, facc[1] + fine_part(3, (2,)))
    pool_plane(1)
    neighbour(pc.at[1], sem_p, 0).start()
    shift_pooled(1)
    shift_pooled(2)
    load_ck.wait()
    load_ct.wait()

    def piece(q, a, b, c):
        return pc[c, q + a, b : b + 8].reshape(256, 128)

    def coarse_part(q, planes):
        taps = [(a, b, c) for a in planes for b in range(3) for c in range(3)]
        acc = None
        for at in range(0, len(taps), 2):
            some = taps[at : at + 2]
            x = jnp.concatenate([piece(q, *tap) for tap in some], axis=1)
            w = jnp.concatenate([ck[9 * a + 3 * b + c] for a, b, c in some], axis=0)
            term = mm(x, w)
            acc = term if acc is None else acc + term
        return acc

    cacc[0] = coarse_part(0, (1, 2))
    cacc[1] = coarse_part(1, (0, 1))
    for t in range(27):
        ckt[t // 3, :, t % 3 * 128 : t % 3 * 128 + 128] = ck[t].T
    def coarse_plane(q):
        neighbour(pc.at[1], sem_p, q).wait_recv()

        @pl.when(i == 63 * q)
        def _():
            pc[1, 3 * q, 1:9] = jnp.zeros((8, 32, 128), BF16)

        shift_pooled(3 * q)
        pre = cacc[q] + coarse_part(q, (0,) if q == 0 else (2,))
        sig = sigmoid(pre)
        act = pre * sig
        outb[q] = act.astype(BF16).reshape(8, 32, 256)
        grad = ct[q].reshape(256, 256).astype(F32)
        cd[q + 1, 1:9] = (grad * (sig + act * (1.0 - sig))).astype(BF16).reshape(8, 32, 256)
        neighbour(cd, sem_c, 1 - q).start()

    coarse_plane(0)
    coarse_plane(1)
    store_out = pltpu.make_async_copy(outb, out_hbm, sem_out)
    store_out.start()

    delta = cd[1:3, 1:9].reshape(512, 256)
    orders = {
        first: mm_nt(picks[k], delta).astype(BF16) for k, first in enumerate(("z", "y"))
    }
    for unit in coarse_units:
        lhs = orders[unit.first]
        for at in range(0, len(unit.taps), 2):
            some = unit.taps[at : at + 2]
            x = jnp.concatenate(
                [
                    pc[t % 3, t // 9 : t // 9 + 2, t // 3 % 3 : t // 3 % 3 + 8].reshape(512, 128)
                    for t in some
                ],
                axis=1,
            )
            term = mm(lhs, x)
            for k in range(len(some)):
                unit.put(at + k, term[:, k * 128 : (k + 1) * 128])
        unit.step_core()

    def back_part(q, planes):
        near, far = None, None
        for a in planes:
            for b in range(3):
                x = cd[q + 2 - a, 2 - b : 10 - b].reshape(256, 256)
                one = mm(x, ckt[3 * a + b, :, 0:256])
                two = mm(x, ckt[3 * a + b, :, 256:384])
                near = one if near is None else near + one
                far = two if far is None else far + two
        return near, far

    cacc[0], spr[0, 0:256] = back_part(0, (0, 1))
    for unit in coarse_units[: len(coarse_units) // 2]:
        unit.step_a()
    cacc[1], spr[1, 0:256] = back_part(1, (1, 2))
    for unit in coarse_units[len(coarse_units) // 2 :]:
        unit.step_a()

    def fine_planes(q):
        neighbour(cd, sem_c, q).wait_recv()

        @pl.when(i == 63 * q)
        def _():
            cd[3 * q, 1:9] = jnp.zeros((8, 32, 256), BF16)

        near, far = back_part(q, (2,) if q == 0 else (0,))
        near, far = near + cacc[q], far + spr[q, 0:256]
        grad = near[:, 128:] + shift_rows(near[:, :128], -1, 32) + shift_rows(far, 1, 32)
        grad = grad.astype(BF16).astype(F32) * 0.125
        spr[q, pl.ds(0, 256, stride=2), :] = grad
        spr[q, pl.ds(1, 256, stride=2), :] = grad
        wide = spr[q]
        for p in (2 * q, 2 * q + 1):
            d = (beside(wide, wide) * slope[p]).astype(BF16)
            for k in range(2):
                dt[k, :, p * 512 : (p + 1) * 512] = mm_nt(picks[2 + k], d).astype(BF16)

    fine_planes(0)
    fine_planes(1)

    def before(a, c):
        return v[c, a : a + 4, 0:8, :, 128:256].reshape(2048, 128)

    def after(a, c):
        return v[c, a : a + 4, 2:10, :, 0:128].reshape(2048, 128)

    def fine_groups(unit, groups, at, count):
        k = 0 if unit.first == "z" else 1
        some = groups[at : at + count]
        if count == 2:
            low = mm(dt[k, 0:128], beside(*(before(*g) for g in some)))
            high = mm(dt[k, 128:256], beside(*(after(*g) for g in some)))
            lows = low[:, :128], low[:, 128:]
            highs = high[:, :128], high[:, 128:]
        else:
            both = mm(dt[k], beside(before(*some[0]), after(*some[0])))
            lows, highs = (both[:128, :128],), (both[128:, 128:],)
        for j, (a, c) in enumerate(some):
            mid = mm(dt[k], v[c, a : a + 4, 1:9].reshape(2048, 256))
            tap = 3 * (at + j)
            unit.put(tap, mid[128:, :128] + lows[j])
            unit.put(tap + 1, mid[:128, :128] + mid[128:, 128:])
            unit.put(tap + 2, mid[:128, 128:] + highs[j])
    one, two, three = fine_units
    groups = [unit[-1] for unit in FINE_UNITS]
    fine_groups(one, groups[0], 0, 2)
    fine_groups(one, groups[0], 2, 2)
    one.step_core()
    for unit in coarse_units:
        unit.step_ring()
    fine_groups(two, groups[1], 0, 2)
    one.step_a()
    fine_groups(two, groups[1], 2, 1)
    two.step_core()
    fine_groups(three, groups[2], 0, 2)
    three.step_core()
    two.step_a()
    for unit in coarse_units:
        unit.step_b()
    three.step_a()
    one.step_b()
    two.step_b()
    three.step_b()
    for unit in coarse_units:
        unit.step_c(coarse_out)
    one.step_c(fine_out)
    two.step_c(fine_out)
    for unit in coarse_units:
        unit.step_d(coarse_out)
    one.step_d(fine_out)
    for side in range(2):
        for e in range(2):
            halo(side, e).wait_send()
        neighbour(pc.at[1], sem_p, side).wait_send()
        neighbour(cd, sem_c, side).wait_send()
    store_out.wait()
    three.step_c(fine_out)


def finish(*refs):
    ins, outs, bufs, sem = refs[:3], refs[3:6], refs[6:9], refs[9]
    reads = [pltpu.make_async_copy(ins[k], bufs[k], sem.at[0, k]) for k in range(3)]
    writes = [pltpu.make_async_copy(bufs[k], outs[k], sem.at[1, k]) for k in range(3)]
    for read in reads:
        read.start()
    for read, write in zip(reads, writes):
        read.wait()
        write.start()
    for write in writes:
        write.wait()


def shards(volumes, fine_kernel, coarse_kernel, cotangent):
    vol = volumes.reshape(4, 8, 2, 64, 128)
    any_spec = pl.BlockSpec(memory_space=pl.ANY)
    vmem = pl.BlockSpec(memory_space=pltpu.VMEM)
    scratch = [
        pltpu.VMEM((3, 6, 10, 64, 256), BF16),
        pltpu.VMEM((27, 128, 128), BF16),
        pltpu.VMEM((27, 128, 256), BF16),
        pltpu.VMEM((2, 8, 32, 256), BF16),
        pltpu.VMEM((4, 512, 256), F32),
        pltpu.VMEM((2, 512, 128), F32),
        pltpu.VMEM((2, 512, 128), F32),
        pltpu.VMEM((3, 4, 10, 32, 128), BF16),
        pltpu.VMEM((4, 10, 32, 256), BF16),
        pltpu.VMEM((2, 256, 256), F32),
        pltpu.VMEM((2, 8, 32, 256), BF16),
        pltpu.VMEM((2, 256, 2048), BF16),
        pltpu.VMEM((2, 512, 256), F32),
        pltpu.VMEM((9, 256, 384), BF16),
        pltpu.VMEM((4, 256, 256), BF16),
        pltpu.SemaphoreType.DMA((5,)),
        pltpu.SemaphoreType.DMA,
        pltpu.SemaphoreType.DMA((2, 2, 2)),
        pltpu.SemaphoreType.DMA((2, 2)),
        pltpu.SemaphoreType.DMA((2, 2)),
    ]
    for *_, taps in COARSE_UNITS:
        scratch += unit_scratch(taps, 4)
    for *_, groups in FINE_UNITS:
        scratch += unit_scratch(fine_taps(groups), 2)
    results = (
        jax.ShapeDtypeStruct((2, 8, 32, 256), BF16),
        jax.ShapeDtypeStruct((2, 3456), F32),
        jax.ShapeDtypeStruct((4, 3456), F32),
    )
    made = pl.pallas_call(
        kernel,
        out_shape=results,
        in_specs=[any_spec] * 4,
        out_specs=(any_spec, vmem, vmem),
        scratch_shapes=scratch,
        compiler_params=pltpu.CompilerParams(
            collective_id=0, has_side_effects=True, vmem_limit_bytes=60 * 2**20
        ),
        name="unet_step",
    )(vol, fine_kernel, coarse_kernel, cotangent[0])
    out, fine, coarse = pl.pallas_call(
        finish,
        out_shape=results,
        in_specs=[any_spec] * 3,
        out_specs=[any_spec] * 3,
        scratch_shapes=[pltpu.VMEM(r.shape, r.dtype) for r in results]
        + [pltpu.SemaphoreType.DMA((2, 3))],
        name="finish",
    )(*made)
    return out[None], fine, coarse


def solution(mesh):
    in_specs = (
        P("sample", "space", None, None, None),
        P(),
        P(),
        P("sample", "space", None, None, None),
    )
    out_specs = (P("sample", "space", None, None, None), P("space", None), P("space", None))
    return jax.shard_map(
        shards, mesh=mesh, in_specs=in_specs, out_specs=out_specs, check_vma=False
    )
```
